32 devices in a mesh: data: 1 (over z), fsdp: 4 (over y), tp: 8 (over x, core).
Axes of the slice: x: 4, y: 4, z: 1, core: 2. Of those that a mesh axis runs over, the one named last changes fastest.
The devices are a block of a 4x4x8 slice.
Arguments:
- hidden: bfloat16 [8192, 6144], P(('data', 'fsdp', 'tp'))
- ln_scale: float32 [6144], replicated
- w_in: bfloat16 [6144, 24576], P('fsdp', 'tp')
- w_out: bfloat16 [24576, 6144], P(('tp', 'fsdp'))
Outputs:
- output: bfloat16 [8192, 6144], P(('data', 'fsdp', 'tp'))
All inputs are finite; a program needn't handle non-finite values.
Results may differ from the reference program's by a relative error of at most 0.00102.
Values are sent between devices in bfloat16 or wider.
A program may use at most 768 MiB of HBM per device.

```python
import jax
import jax.numpy as jnp
from jax import lax

TOKENS_DEV = 256
MODEL_DIM = 6144
FFN_DIM = 24576
GROUP_DEVICES = 32
GROUP_ROWS = GROUP_DEVICES * TOKENS_DEV
LN_EPS = 1e-6


def setup_inputs(seed: int = 0, part: int = 0) -> dict:
    base_key = jax.random.key(seed)
    key_rows, key_gain, key_in, key_out = jax.random.split(base_key, 4)
    key_rows = jax.random.fold_in(key_rows, part)
    hidden = jax.random.normal(key_rows, (GROUP_ROWS, MODEL_DIM), jnp.float32).astype(jnp.bfloat16)
    ln_scale = 1.0 + 0.3 * jax.random.normal(key_gain, (MODEL_DIM,), jnp.float32)
    w_in = (jax.random.normal(key_in, (MODEL_DIM, FFN_DIM), jnp.float32) * MODEL_DIM ** -0.5).astype(jnp.bfloat16)
    w_out = (jax.random.normal(key_out, (FFN_DIM, MODEL_DIM), jnp.float32) * (1.5 * FFN_DIM ** -0.5)).astype(jnp.bfloat16)
    return {"hidden": hidden, "ln_scale": ln_scale, "w_in": w_in, "w_out": w_out}


def layer_norm(row_block, ln_scale):
    block_f32 = row_block.astype(jnp.float32)
    centered = block_f32 - jnp.mean(block_f32, axis=-1, keepdims=True)
    var_row = jnp.mean(centered * centered, axis=-1, keepdims=True)
    return (centered * lax.rsqrt(var_row + LN_EPS) * ln_scale).astype(jnp.bfloat16)


def reference(hidden, ln_scale, w_in, w_out):
    normed = layer_norm(hidden, ln_scale).reshape(GROUP_DEVICES, TOKENS_DEV, MODEL_DIM)

    def mlp_block(row_block):
        pre_act = jnp.dot(row_block, w_in, preferred_element_type=jnp.float32)
        act_out = jax.nn.gelu(pre_act, approximate=True).astype(jnp.bfloat16)
        return jnp.dot(act_out, w_out, preferred_element_type=jnp.float32)

    mlp_out = lax.map(mlp_block, normed).reshape(GROUP_ROWS, MODEL_DIM)
    return (hidden.astype(jnp.float32) + mlp_out).astype(jnp.bfloat16)
```

```python
import functools

import jax
import jax.numpy as jnp
from jax import lax
from jax.experimental import pallas as pl
from jax.experimental.pallas import tpu as pltpu
from jax.sharding import PartitionSpec as P

LN_EPS = 1e-6
CHUNKS = 12
F32 = jnp.float32
BF16 = jnp.bfloat16


def mlp_kernel(
    n_tp, n_y, N, hid_ref, scale_ref, win_ref, wout_ref, out_ref, gin_ref, gout_ref,
    u_all, h, wbuf, hid_v, own, sibst, sibr, far, near,
    ws_sem, wr_sem, fs_sem, fr_sem, ld_sem, hid_sem, out_sem,
    us_sem, ur_sem, uf_s, uf_r, ub_s, ub_r,
    sb_s, sb_r, far_s, far_r, near_s, near_r,
):
    R, D = hid_v.shape
    Fb = h.shape[1]
    dk, fs = win_ref.shape[0], wout_ref.shape[0]
    cf, cd = Fb // N, D // N
    n_x = n_tp // 2
    t = lax.axis_index("tp")
    y = lax.axis_index("fsdp")
    x, c = lax.div(t, 2), lax.rem(t, 2)
    xr, xl, xf = lax.rem(x + 1, n_x), lax.rem(x + n_x - 1, n_x), lax.rem(x + 2, n_x)
    tr, tl, tf = xr * 2 + c, xl * 2 + c, xf * 2 + c
    tsib = x * 2 + 1 - c
    yr, yl, yf = lax.rem(y + 1, n_y), lax.rem(y + n_y - 1, n_y), lax.rem(y + 2, n_y)
    ynb = ({"fsdp": yr}, {"fsdp": yl})
    xnb = ({"tp": tr}, {"tp": tl})
    sib = {"tp": tsib}

    def remote(src, dst, s, r, dev):
        return pltpu.make_async_remote_copy(
            src_ref=src, dst_ref=dst, send_sem=s, recv_sem=r, device_id=dev, device_id_type=pl.DeviceIdType.MESH
        )

    def cols(k, n):
        return pl.ds(pl.multiple_of(k * n, 128), n)

    def own_copy(ph, k, d):
        if ph == 0:
            src, dst = win_ref.at[:, cols(k, cf)], gin_ref.at[y, :, cols(k, cf)]
        else:
            src, dst = wout_ref.at[:, cols(k, cd)], gout_ref.at[y, :, cols(k, cd)]
        return remote(src, dst, ws_sem.at[ph, lax.rem(k, 2), d], wr_sem.at[ph, k, d], ynb[d])

    def fwd_copy(ph, k, d):
        o = (yl, yr)[d]
        if ph == 0:
            ref = gin_ref.at[o, pl.ds(d * (dk // 2), dk // 2), cols(k, cf)]
        else:
            ref = gout_ref.at[o, pl.ds(d * (fs // 2), fs // 2), cols(k, cd)]
        return remote(ref, ref, fs_sem.at[ph, lax.rem(k, 2), d], fr_sem.at[ph, k, d], ynb[d])

    def start_own(ph, k):
        for d in range(2):
            @pl.when(k >= 2)
            def _():
                own_copy(ph, k - 2, d).wait_send()

            own_copy(ph, k, d).start()

    def forward(ph, k):
        for d in range(2):
            own_copy(ph, k, d).wait_recv()

            @pl.when(k >= 2)
            def _():
                fwd_copy(ph, k - 2, d).wait_send()

            fwd_copy(ph, k, d).start()

    def wait_far(ph, k):
        for d in range(2):
            fwd_copy(ph, k, d).wait_recv()

    def pump(ph, k):
        for fn, a in ((start_own, 2), (forward, 1)):
            @pl.when(k + a < N)
            def _():
                fn(ph, k + a)

            if ph == 0:
                @pl.when(k + a >= N)
                def _():
                    fn(1, k + a - N)
        wait_far(ph, k)

    def drain_sends(ph):
        for k in (N - 2, N - 1):
            for d in range(2):
                own_copy(ph, k, d).wait_send()
                fwd_copy(ph, k, d).wait_send()

    barrier = pltpu.get_barrier_semaphore()
    for dev in (*ynb, *xnb, sib):
        pl.semaphore_signal(barrier, inc=1, device_id=dev, device_id_type=pl.DeviceIdType.MESH)
    hid_load = pltpu.make_async_copy(hid_ref, hid_v, hid_sem)
    hid_load.start()
    pl.semaphore_wait(barrier, 5)

    start_own(0, 0)
    start_own(0, 1)

    hid_load.wait()
    TR = 16

    @pl.loop(0, R // TR)
    def _(i):
        rows = pl.ds(pl.multiple_of(i * TR, TR), TR)
        v = hid_v[rows, :].astype(F32)
        cen = v - jnp.mean(v, axis=-1, keepdims=True)
        var = jnp.mean(cen * cen, axis=-1, keepdims=True)
        u = (cen * lax.rsqrt(var + LN_EPS) * scale_ref[...]).astype(BF16)
        u_all[pl.ds(pl.multiple_of(t * R + i * TR, TR), TR), :] = u

    hr = R // 2

    def urows(tt, part):
        return u_all.at[pl.ds(pl.multiple_of(tt * R + part * hr, 16), hr), :]

    def u_copy(d, part):
        return remote(urows(t, part), urows(t, part), us_sem.at[d, part], ur_sem.at[d, part], xnb[d])

    def u_fwd(d):
        ref = urows((tl, tr)[d], d)
        return remote(ref, ref, uf_s.at[d], uf_r.at[d], xnb[d])

    SIB = ((t, 0), (t, 1), (tl, 0), (tr, 1), (tl, 1), (tr, 0), (tf, 0), (tf, 1))

    def u_sib(i):
        ref = urows(*SIB[i])
        return remote(ref, ref, ub_s.at[i], ub_r.at[i], sib)

    for i in range(2):
        u_copy(0, i).start()
        u_copy(1, 1 - i).start()
    u_sib(0).start()
    u_sib(1).start()

    forward(0, 0)
    pump(0, 0)
    u_copy(0, 0).wait_recv()
    u_fwd(0).start()
    u_copy(1, 1).wait_recv()
    u_fwd(1).start()
    u_sib(2).start()
    u_sib(3).start()
    pump(0, 1)
    u_copy(0, 1).wait_recv()
    u_sib(4).start()
    u_copy(1, 0).wait_recv()
    u_sib(5).start()
    pump(0, 2)
    for d in range(2):
        u_fwd(d).wait_recv()
        u_sib(6 + d).start()

    def up_chunk(k):
        loads = []
        for i, o in enumerate((y, yl, yr, yf)):
            src = win_ref if i == 0 else gin_ref.at[o]
            dst = wbuf.at[
                pl.ds(pl.multiple_of(lax.rem(o, 2) * dk, 16), dk),
                pl.ds(pl.multiple_of(lax.div(o, 2) * cf, 128), cf),
            ]
            loads.append(pltpu.make_async_copy(src.at[:, cols(k, cf)], dst, ld_sem.at[i]))
        for cp in loads:
            cp.start()
        for cp in loads:
            cp.wait()

        @pl.loop(0, n_tp)
        def _(b):
            rows = pl.ds(pl.multiple_of(b * R, 16), R)
            pre = jnp.dot(u_all[rows, : D // 2], wbuf[:, :cf], preferred_element_type=F32)
            pre += jnp.dot(u_all[rows, D // 2 :], wbuf[:, cf:], preferred_element_type=F32)
            h[rows, cols(k, cf)] = jax.nn.gelu(pre, approximate=True).astype(BF16)

    pump(0, 3)
    for i in range(8):
        u_sib(i).wait_recv()

    @pl.loop(0, 3)
    def _(i):
        @pl.when(i > 0)
        def _():
            pump(0, i + 3)

        @pl.loop(0, 2)
        def _(b):
            up_chunk(2 * i + b)

    @pl.loop(6, N)
    def _(k):
        pump(0, k)
        up_chunk(k)

    drain_sends(0)
    for d in range(2):
        u_fwd(d).wait_send()
        for part in range(2):
            u_copy(d, part).wait_send()
    for i in range(8):
        u_sib(i).wait_send()

    hc = cd // 2

    def sib_copy(j):
        s = lax.rem(j, 2)
        return remote(sibst, sibr.at[s], sb_s, sb_r.at[s], sib)

    def far_copy(j, d):
        s = lax.rem(j, 2)
        return remote(
            own.at[lax.rem(j, 3), xf, :, pl.ds(d * hc, hc)], far.at[s, d], far_s.at[s, d], far_r.at[s, d], xnb[d]
        )

    def near_copy(j, d):
        s = lax.rem(j, 2)
        return remote(own.at[lax.rem(j, 3), (xr, xl)[d]], near.at[s, d], near_s.at[s, d], near_r.at[s, d], xnb[d])

    def out_copy(j):
        return pltpu.make_async_copy(hid_v.at[:, cols(j, cd)], out_ref.at[:, cols(j, cd)], out_sem.at[j])

    def down_chunk(j):
        loads = []
        for i, o in enumerate((y, yl, yr, yf)):
            src = wout_ref if i == 0 else gout_ref.at[o]
            dst = wbuf.at[pl.ds(pl.multiple_of(o * fs, 16), fs), :]
            loads.append(pltpu.make_async_copy(src.at[:, cols(j, cd)], dst, ld_sem.at[i]))
        for cp in loads:
            cp.start()

        @pl.when(j >= 1)
        def _():
            sib_copy(j - 1).wait_send()

        for cp in loads:
            cp.wait()

        @pl.loop(0, n_x)
        def _(b):
            rows = pl.ds(pl.multiple_of((b * 2 + 1 - c) * R, 16), R)
            sibst[b] = jnp.dot(h[rows, :], wbuf[...], preferred_element_type=F32)

        sib_copy(j).start()
        s3 = lax.rem(j, 3)

        @pl.loop(0, n_x)
        def _(b):
            rows = pl.ds(pl.multiple_of((b * 2 + c) * R, 16), R)
            own[s3, b] = jnp.dot(h[rows, :], wbuf[...], preferred_element_type=F32)

    def reduce_pair(j):
        s3, s2 = lax.rem(j, 3), lax.rem(j, 2)
        sib_copy(j).wait_recv()

        @pl.loop(0, n_x)
        def _(b):
            own[s3, b] = own[s3, b] + sibr[s2, b]

        for d in range(2):
            @pl.when(j >= 2)
            def _():
                far_copy(j - 2, d).wait_send()

            far_copy(j, d).start()

    def reduce_far(j):
        s3, s2 = lax.rem(j, 3), lax.rem(j, 2)
        for d in range(2):
            half = slice(d * hc, (d + 1) * hc)
            far_copy(j, d).wait_recv()
            b = (xr, xl)[d]
            own[s3, b, :, half] = own[s3, b, :, half] + far[s2, d]
        for d in range(2):
            @pl.when(j >= 2)
            def _():
                near_copy(j - 2, d).wait_send()

            near_copy(j, d).start()

    def finish(j):
        s3, s2 = lax.rem(j, 3), lax.rem(j, 2)
        for d in range(2):
            near_copy(j, d).wait_recv()
        tot = own[s3, x] + near[s2, 0] + near[s2, 1]
        hid_v[:, cols(j, cd)] = (hid_v[:, cols(j, cd)].astype(F32) + tot).astype(BF16)
        out_copy(j).start()

    @pl.loop(0, N)
    def _(j):
        pump(1, j)

        @pl.when(j >= 1)
        def _():
            reduce_far(j - 1)

        @pl.when(j >= 2)
        def _():
            finish(j - 2)

        down_chunk(j)
        reduce_pair(j)

    reduce_far(N - 1)
    finish(N - 2)
    finish(N - 1)

    drain_sends(1)
    sib_copy(N - 1).wait_send()
    for d in range(2):
        for j in (N - 2, N - 1):
            far_copy(j, d).wait_send()
            near_copy(j, d).wait_send()
    for j in range(N):
        out_copy(j).wait()


def make_local(n_tp, n_y, N):
    def local_mlp(hidden, ln_scale, w_in, w_out):
        R, D = hidden.shape
        dk, Fb = w_in.shape
        fs = w_out.shape[0]
        cd = D // N
        any_spec = pl.BlockSpec(memory_space=pl.ANY)
        dma = pltpu.SemaphoreType.DMA
        flops = 4 * n_tp * R * D * Fb
        out, _, _ = pl.pallas_call(
            functools.partial(mlp_kernel, n_tp, n_y, N),
            out_shape=(
                jax.ShapeDtypeStruct((R, D), BF16),
                jax.ShapeDtypeStruct((n_y, dk, Fb), BF16),
                jax.ShapeDtypeStruct((n_y, fs, D), BF16),
            ),
            in_specs=[any_spec, pl.BlockSpec(memory_space=pltpu.VMEM), any_spec, any_spec],
            out_specs=(any_spec, any_spec, any_spec),
            scratch_shapes=[
                pltpu.VMEM((n_tp * R, D), BF16),
                pltpu.VMEM((n_tp * R, Fb), BF16),
                pltpu.VMEM((Fb, cd), BF16),
                pltpu.VMEM((R, D), BF16),
                pltpu.VMEM((3, n_tp // 2, R, cd), F32),
                pltpu.VMEM((n_tp // 2, R, cd), F32),
                pltpu.VMEM((2, n_tp // 2, R, cd), F32),
                pltpu.VMEM((2, 2, R, cd // 2), F32),
                pltpu.VMEM((2, 2, R, cd), F32),
                dma((2, 2, 2)), dma((2, N, 2)), dma((2, 2, 2)), dma((2, N, 2)), dma((4,)), dma, dma((N,)),
                dma((2, 2)), dma((2, 2)), dma((2,)), dma((2,)), dma((8,)), dma((8,)),
                dma, dma((2,)), dma((2, 2)), dma((2, 2)), dma((2, 2)), dma((2, 2)),
            ],
            compiler_params=pltpu.CompilerParams(
                collective_id=0, has_side_effects=True, vmem_limit_bytes=67043328
            ),
            cost_estimate=pl.CostEstimate(flops=flops, bytes_accessed=8 * D * Fb, transcendentals=0),
            name="mlp",
        )(hidden, ln_scale.reshape(1, D), w_in, w_out)
        return out

    return local_mlp


def solution(mesh):
    return jax.shard_map(
        make_local(mesh.shape["tp"], mesh.shape["fsdp"], CHUNKS),
        mesh=mesh,
        in_specs=(P(("data", "fsdp", "tp"), None), P(None), P("fsdp", "tp"), P(("tp", "fsdp"), None)),
        out_specs=P(("data", "fsdp", "tp"), None),
        check_vma=False,
    )
```

```python
import functools

import jax
import jax.numpy as jnp
from jax import lax
from jax.experimental import pallas as pl
from jax.experimental.pallas import tpu as pltpu
from jax.sharding import PartitionSpec as P

LN_EPS = 1e-6
CHUNKS = 24
F32 = jnp.float32
BF16 = jnp.bfloat16
SLOTS = 4


def split_rows(R):
    return R * 9 // 16 // 16 * 16


def mlp_kernel(
    n_tp, n_y, N, hid_ref, scale_ref, win_ref, wout_ref, out_ref, u_ref, gout_ref,
    wb, h, ub, hid_v, own, sibst, sibr, yey, fx, nx, fy, ny, yex,
    hid_sem, ust_sem, ld_sem, w2_sem, out_sem,
    d_s, d_r, s_s, s_r, f_s, f_r, wo_s, wo_r,
    uy_s, uy_r, ux_s, ux_r, uf_s, uf_r, ub_s, ub_r,
    sb_s, sb_r, yey_s, yey_r, fx_s, fx_r, nx_s, nx_r, fy_s, fy_r, ny_s, ny_r, yex_s, yex_r,
):
    R, D = hid_v.shape
    sub = wout_ref.shape[0]
    dk = win_ref.shape[0]
    K1 = 6
    cf, cd = sub // 3, D // N
    F2 = 2 * sub
    n_x = n_tp // 2
    RX = split_rows(R)
    hx, hy = RX // 2, (R - RX) // 2
    t = lax.axis_index("tp")
    y = lax.axis_index("fsdp")
    x, c = lax.div(t, 2), lax.rem(t, 2)
    xr, xl, xf = lax.rem(x + 1, n_x), lax.rem(x + n_x - 1, n_x), lax.rem(x + 2, n_x)
    tr, tl, tf = xr * 2 + c, xl * 2 + c, xf * 2 + c
    tsib = x * 2 + 1 - c
    yp = lax.div(y, 2) * 2 + 1 - lax.rem(y, 2)
    yd = n_y - 1 - y
    yo = n_y - 1 - yp
    pair, other, sib = {"fsdp": yp}, {"fsdp": yd}, {"tp": tsib}
    xnb = ({"tp": tr}, {"tp": tl})

    def remote(src, dst, s, r, dev):
        return pltpu.make_async_remote_copy(
            src_ref=src, dst_ref=dst, send_sem=s, recv_sem=r, device_id=dev, device_id_type=pl.DeviceIdType.MESH
        )

    def cols(k, n):
        return pl.ds(pl.multiple_of(k * n, 128), n)

    def wrows(o):
        return pl.ds(pl.multiple_of(o * dk, 16), dk)

    def sseq(m):
        return lax.rem(m, 2) * 3 + lax.div(m, 2)

    def kseq(m):
        return lax.rem(m + 1, 2) * 3 + lax.div(m, 2)

    def win_cols(first, second, k):
        s = jnp.where(k < 3, first, second) if not isinstance(k, int) else (first if k < 3 else second)
        return pl.ds(pl.multiple_of(s * sub + lax.rem(k, 3) * cf, 128), cf)

    def own_w(k):
        return pltpu.make_async_copy(
            win_ref.at[:, win_cols(y, yd, k)], wb.at[wrows(y), cols(k, cf)], ld_sem.at[2 + k]
        )

    def d_copy(k):
        return remote(
            win_ref.at[:, win_cols(yd, y, k)], wb.at[wrows(y), cols(k, cf)], d_s.at[k], d_r.at[k], other
        )

    def s_copy(k):
        return remote(
            win_ref.at[:, win_cols(yp, yo, k)], wb.at[wrows(y), cols(k, cf)], s_s.at[k], s_r.at[k], pair
        )

    def f_copy(k):
        kk = lax.rem(k + 3, K1)
        return remote(
            wb.at[wrows(yp), cols(k, cf)], wb.at[wrows(yp), cols(kk, cf)], f_s.at[kk], f_r.at[kk], other
        )

    def f_recv(k):
        return remote(wb.at[wrows(yo), cols(k, cf)], wb.at[wrows(yo), cols(k, cf)], f_s.at[k], f_r.at[k], other)

    def wo_copy(j):
        return remote(wout_ref.at[:, cols(j, cd)], gout_ref.at[:, cols(j, cd)], wo_s.at[j], wo_r.at[j], other)

    barrier = pltpu.get_barrier_semaphore()
    for dev in (pair, other, *xnb, sib):
        pl.semaphore_signal(barrier, inc=1, device_id=dev, device_id_type=pl.DeviceIdType.MESH)
    hid_load = pltpu.make_async_copy(hid_ref, hid_v, hid_sem)
    hid_load.start()
    pl.semaphore_wait(barrier, 5)

    s_copy(0).start()
    for m in range(K1):
        d_copy(((m + 1) % 2) * 3 + m // 2).start()

    hid_load.wait()
    TR = 16

    @pl.loop(0, R // TR)
    def _(i):
        rows = pl.ds(pl.multiple_of(i * TR, TR), TR)
        v = hid_v[rows, :].astype(F32)
        cen = v - jnp.mean(v, axis=-1, keepdims=True)
        var = jnp.mean(cen * cen, axis=-1, keepdims=True)
        ub[0, rows, :] = (cen * lax.rsqrt(var + LN_EPS) * scale_ref[...]).astype(BF16)

    u_store = pltpu.make_async_copy(ub.at[0], u_ref.at[0, t], ust_sem)
    u_store.start()
    u_store.wait()

    hr = R // 2

    def urows(yy, tt, part):
        return u_ref.at[yy, tt, pl.ds(part * hr, hr), :]

    def u_pair(part):
        return remote(urows(0, t, part), urows(1, t, part), uy_s.at[part], uy_r.at[part], pair)

    def u_copy(yy, d, part):
        ref = urows(yy, t, part)
        return remote(ref, ref, ux_s.at[yy, d, part], ux_r.at[yy, d, part], xnb[d])

    def u_fwd(yy, d):
        ref = urows(yy, (tl, tr)[d], d)
        return remote(ref, ref, uf_s.at[yy, d], uf_r.at[yy, d], xnb[d])

    SIB = ((t, 0), (t, 1), (tl, 0), (tr, 1), (tl, 1), (tr, 0), (tf, 0), (tf, 1))

    def u_sib(yy, i):
        ref = urows(yy, *SIB[i])
        return remote(ref, ref, ub_s.at[yy, i], ub_r.at[yy, i], sib)

    def u_start(yy):
        for i in range(2):
            u_copy(yy, 0, i).start()
            u_copy(yy, 1, 1 - i).start()

    def u_first(yy):
        u_copy(yy, 0, 0).wait_recv()
        u_fwd(yy, 0).start()
        u_copy(yy, 1, 1).wait_recv()
        u_fwd(yy, 1).start()
        u_sib(yy, 2).start()
        u_sib(yy, 3).start()

    def u_second(yy):
        u_copy(yy, 0, 1).wait_recv()
        u_sib(yy, 4).start()
        u_copy(yy, 1, 0).wait_recv()
        u_sib(yy, 5).start()

    def u_third(yy):
        for d in range(2):
            u_fwd(yy, d).wait_recv()
            u_sib(yy, 6 + d).start()

    u_start(0)
    for i in range(2):
        u_pair(i).start()
        u_sib(0, i).start()
    for m in range(1, K1):
        s_copy((m % 2) * 3 + m // 2).start()
    for k in range(K1):
        own_w(k).start()

    def block(i):
        yy = lax.div(i, n_tp)
        m = lax.div(lax.rem(i, n_tp), 2)
        off = lax.div(m * (m + 1), 2)
        return yy, lax.rem(x + off, n_x) * 2 + lax.rem(i, 2)

    def u_load(i):
        yy, tt = block(i)
        return pltpu.make_async_copy(u_ref.at[yy, tt], ub.at[lax.rem(i, 2)], ld_sem.at[lax.rem(i, 2)])

    def up(i0, i1, m0, m1):
        u_load(i0).start()

        @pl.loop(i0, i1)
        def _(i):
            @pl.when(i + 1 < i1)
            def _():
                u_load(i + 1).start()

            u_load(i).wait()
            yy, tt = block(i)
            rows = pl.ds(pl.multiple_of((yy * n_tp + tt) * R, 16), R)

            @pl.loop(m0, m1)
            def _(m):
                k = kseq(m)
                pre = jnp.dot(ub[lax.rem(i, 2)], wb[:, cols(k, cf)], preferred_element_type=F32)
                h[rows, cols(k, cf)] = jax.nn.gelu(pre, approximate=True).astype(BF16)

    def s_event(m):
        s_copy(sseq(m)).wait_recv()
        f_copy(sseq(m)).start()

    def w_ready(m):
        k = kseq(m)
        d_copy(k).wait_recv()
        f_recv(k).wait_recv()

    s_event(0)
    u_first(0)
    u_second(0)
    for i in range(2):
        u_pair(i).wait_recv()
    u_start(1)
    for i in range(2):
        u_sib(1, i).start()
    s_event(1)
    u_third(0)
    for i in range(8):
        u_sib(0, i).wait_recv()
    for i in range(2):
        u_sib(1, i).wait_recv()
    for k in range(K1):
        own_w(k).wait()

    @pl.loop(0, 4)
    def _(m):
        s_event(m + 2)
        w_ready(m)

        @pl.when(m == 2)
        def _():
            u_first(1)

        up(0, 10, m, m + 1)

    for j in range(SLOTS):
        wo_copy(j).start()
    u_second(1)
    for i in range(2, 6):
        u_sib(1, i).wait_recv()
    up(10, 14, 0, 4)

    @pl.loop(4, K1)
    def _(m):
        w_ready(m)
        up(0, 14, m, m + 1)

    u_third(1)
    for i in range(6, 8):
        u_sib(1, i).wait_recv()
    up(14, 16, 0, K1)

    for k in range(K1):
        f_copy(k).wait_send()
        d_copy(k).wait_send()
        s_copy(k).wait_send()

    def s2(j):
        return lax.rem(j, 2)

    def s4(j):
        return lax.rem(j, SLOTS)

    def sib_copy(j):
        return remote(sibst, sibr.at[s2(j)], sb_s, sb_r.at[s2(j)], sib)

    def yey_copy(j):
        return remote(own.at[s4(j), 1, :, pl.ds(RX, R - RX)], yey.at[s4(j)], yey_s.at[s2(j)], yey_r.at[s4(j)], pair)

    def yex_copy(j):
        return remote(own.at[s4(j), 1, x, pl.ds(0, RX)], yex.at[s4(j)], yex_s.at[s2(j)], yex_r.at[s4(j)], pair)

    def fx_copy(j, d):
        src = own.at[s4(j), :, xf, pl.ds(d * hx, hx)]
        return remote(src, fx.at[s4(j), d], fx_s.at[s2(j), d], fx_r.at[s4(j), d], xnb[d])

    def nx_copy(j, d):
        src = own.at[s4(j), :, (xr, xl)[d], pl.ds(0, RX)]
        return remote(src, nx.at[s4(j), d], nx_s.at[s2(j), d], nx_r.at[s4(j), d], xnb[d])

    def fy_copy(j, d):
        src = own.at[s4(j), 0, xf, pl.ds(RX + d * hy, hy)]
        return remote(src, fy.at[s4(j), d], fy_s.at[s2(j), d], fy_r.at[s4(j), d], xnb[d])

    def ny_copy(j, d):
        src = own.at[s4(j), 0, (xr, xl)[d], pl.ds(RX, R - RX)]
        return remote(src, ny.at[s4(j), d], ny_s.at[s2(j), d], ny_r.at[s4(j), d], xnb[d])

    def out_copy(j):
        return pltpu.make_async_copy(hid_v.at[:, cols(j, cd)], out_ref.at[:, cols(j, cd)], out_sem.at[j])

    def send(copy, j, *a):
        @pl.when(j >= 2)
        def _():
            copy(j - 2, *a).wait_send()

        copy(j, *a).start()

    def w2_loads(j):
        dst = wb.at[:, cols(s2(j), cd)]
        return (
            pltpu.make_async_copy(wout_ref.at[:, cols(j, cd)], dst.at[pl.ds(0, sub)], w2_sem.at[s2(j), 0]),
            pltpu.make_async_copy(gout_ref.at[:, cols(j, cd)], dst.at[pl.ds(sub, sub)], w2_sem.at[s2(j), 1]),
        )

    def fetch(j):
        wo_copy(j).wait_recv()
        for cp in w2_loads(j):
            cp.start()

    def down(j):
        for cp in w2_loads(j):
            cp.wait()

        @pl.when(j + 1 < N)
        def _():
            fetch(j + 1)

        @pl.when(j >= 1)
        def _():
            sib_copy(j - 1).wait_send()

        def part(i, cc):
            yy, xx = lax.div(i, n_x), lax.rem(i, n_x)
            rows = pl.ds(pl.multiple_of((yy * n_tp + xx * 2 + cc) * R, 16), R)
            return jnp.dot(h[rows, :], wb[:F2, cols(s2(j), cd)], preferred_element_type=F32)

        @pl.loop(0, 2 * n_x)
        def _(i):
            sibst[lax.div(i, n_x), lax.rem(i, n_x)] = part(i, 1 - c)

        sib_copy(j).start()

        @pl.loop(0, 2 * n_x)
        def _(i):
            own[s4(j), lax.div(i, n_x), lax.rem(i, n_x)] = part(i, c)

    def stage1(j):
        sib_copy(j).wait_recv()

        @pl.loop(0, 2 * n_x)
        def _(i):
            yy, xx = lax.div(i, n_x), lax.rem(i, n_x)
            own[s4(j), yy, xx] = own[s4(j), yy, xx] + sibr[s2(j), yy, xx]

        send(yey_copy, j)
        for d in range(2):
            send(fx_copy, j, d)

    def stage2(j):
        s = s4(j)
        for d in range(2):
            fx_copy(j, d).wait_recv()
            b, rows = (xr, xl)[d], slice(d * hx, (d + 1) * hx)
            for yy in range(2):
                own[s, yy, b, rows] = own[s, yy, b, rows] + fx[s, d, yy]
        for d in range(2):
            send(nx_copy, j, d)
        yey_copy(j).wait_recv()

        @pl.loop(0, n_x)
        def _(i):
            own[s, 0, i, RX:] = own[s, 0, i, RX:] + yey[s, i]

        for d in range(2):
            send(fy_copy, j, d)

    def stage3(j):
        s = s4(j)
        for d in range(2):
            fy_copy(j, d).wait_recv()
            b, rows = (xr, xl)[d], slice(RX + d * hy, RX + (d + 1) * hy)
            own[s, 0, b, rows] = own[s, 0, b, rows] + fy[s, d]
        for d in range(2):
            ny_copy(j, d).start()
        for d in range(2):
            nx_copy(j, d).wait_recv()
        for yy in (1, 0):
            own[s, yy, x, :RX] = own[s, yy, x, :RX] + nx[s, 0, yy] + nx[s, 1, yy]
        yex_copy(j).start()

    def stage4(j):
        s = s4(j)
        for d in range(2):
            ny_copy(j, d).wait_recv()
        lo = own[s, 0, x, RX:] + ny[s, 0] + ny[s, 1]
        hid_v[RX:, cols(j, cd)] = (hid_v[RX:, cols(j, cd)].astype(F32) + lo).astype(BF16)
        yex_copy(j).wait_recv()
        hi = own[s, 0, x, :RX] + yex[s]
        hid_v[:RX, cols(j, cd)] = (hid_v[:RX, cols(j, cd)].astype(F32) + hi).astype(BF16)
        out_copy(j).start()
        yex_copy(j).wait_send()
        for d in range(2):
            ny_copy(j, d).wait_send()

    fetch(0)

    @pl.loop(0, N + 3)
    def _(j):
        @pl.when(j + SLOTS < N)
        def _():
            wo_copy(j + SLOTS).start()

        @pl.when(j < N)
        def _():
            down(j)
            stage1(j)

        @pl.when(jnp.logical_and(j >= 1, j < N + 1))
        def _():
            stage2(j - 1)

        @pl.when(jnp.logical_and(j >= 2, j < N + 2))
        def _():
            stage3(j - 2)

        @pl.when(j >= 3)
        def _():
            stage4(j - 3)

    for yy in range(2):
        for d in range(2):
            u_fwd(yy, d).wait_send()
            for part in range(2):
                u_copy(yy, d, part).wait_send()
        for i in range(8):
            u_sib(yy, i).wait_send()
    for part in range(2):
        u_pair(part).wait_send()
    sib_copy(N - 1).wait_send()
    for j in (N - 2, N - 1):
        yey_copy(j).wait_send()
        for d in range(2):
            for copy in (fx_copy, nx_copy, fy_copy):
                copy(j, d).wait_send()

    @pl.loop(0, N)
    def _(j):
        wo_copy(j).wait_send()
        out_copy(j).wait()


def make_local(n_tp, n_y, N):
    def local_mlp(hidden, ln_scale, w_in, w_out):
        R, D = hidden.shape
        sub = w_out.shape[0]
        cd = D // N
        n_x = n_tp // 2
        RX = split_rows(R)
        any_spec = pl.BlockSpec(memory_space=pl.ANY)
        dma = pltpu.SemaphoreType.DMA
        vm = pltpu.VMEM
        S = SLOTS
        out, _, _ = pl.pallas_call(
            functools.partial(mlp_kernel, n_tp, n_y, N),
            out_shape=(
                jax.ShapeDtypeStruct((R, D), BF16),
                jax.ShapeDtypeStruct((2, n_tp, R, D), BF16),
                jax.ShapeDtypeStruct((sub, D), BF16),
            ),
            in_specs=[any_spec, pl.BlockSpec(memory_space=vm), any_spec, any_spec],
            out_specs=(any_spec, any_spec, any_spec),
            scratch_shapes=[
                vm((D, 2 * sub), BF16),
                vm((2 * n_tp * R, 2 * sub), BF16),
                vm((2, R, D), BF16),
                vm((R, D), BF16),
                vm((S, 2, n_x, R, cd), F32),
                vm((2, n_x, R, cd), F32),
                vm((2, 2, n_x, R, cd), F32),
                vm((S, n_x, R - RX, cd), F32),
                vm((S, 2, 2, RX // 2, cd), F32),
                vm((S, 2, 2, RX, cd), F32),
                vm((S, 2, (R - RX) // 2, cd), F32),
                vm((S, 2, R - RX, cd), F32),
                vm((S, RX, cd), F32),
                dma, dma, dma((8,)), dma((2, 2)), dma((N,)),
                dma((6,)), dma((6,)), dma((6,)), dma((6,)), dma((6,)), dma((6,)), dma((N,)), dma((N,)),
                dma((2,)), dma((2,)), dma((2, 2, 2)), dma((2, 2, 2)), dma((2, 2)), dma((2, 2)), dma((2, 8)), dma((2, 8)),
                dma, dma((2,)), dma((2,)), dma((S,)), dma((2, 2)), dma((S, 2)), dma((2, 2)), dma((S, 2)),
                dma((2, 2)), dma((S, 2)), dma((2, 2)), dma((S, 2)), dma((2,)), dma((S,)),
            ],
            compiler_params=pltpu.CompilerParams(
                collective_id=0, has_side_effects=True, vmem_limit_bytes=67043328
            ),
            cost_estimate=pl.CostEstimate(
                flops=4 * n_tp * R * D * w_in.shape[1], bytes_accessed=8 * D * w_in.shape[1], transcendentals=0
            ),
            name="mlp",
        )(hidden, ln_scale.reshape(1, D), w_in, w_out)
        return out

    return local_mlp


def solution(mesh):
    return jax.shard_map(
        make_local(mesh.shape["tp"], mesh.shape["fsdp"], CHUNKS),
        mesh=mesh,
        in_specs=(P(("data", "fsdp", "tp"), None), P(None), P("fsdp", "tp"), P(("tp", "fsdp"), None)),
        out_specs=P(("data", "fsdp", "tp"), None),
        check_vma=False,
    )
```

```python
import functools

import jax
import jax.numpy as jnp
from jax import lax
from jax.experimental import pallas as pl
from jax.experimental.pallas import tpu as pltpu
from jax.sharding import PartitionSpec as P

LN_EPS = 1e-6
CHUNKS = 24
F32 = jnp.float32
BF16 = jnp.bfloat16
SLOTS = 4


def split_rows(R):
    return R * 9 // 16 // 16 * 16


def mlp_kernel(
    n_tp, n_y, N, hid_ref, scale_ref, win_ref, wout_ref, out_ref, u_ref, gout_ref,
    wb, h, ub, hid_v, own, sibst, sibr, yey, fx, nx, fy, ny, yex,
    hid_sem, ust_sem, ld_sem, ow_sem, w2_sem, out_sem,
    d_s, d_r, s_s, s_r, f_s, f_r, wo_s, wo_r,
    uy_s, uy_r, ux_s, ux_r, uf_s, uf_r, ub_s, ub_r,
    sb_s, sb_r, yey_s, yey_r, fx_s, fx_r, nx_s, nx_r, fy_s, fy_r, ny_s, ny_r, yex_s, yex_r,
):
    R, D = hid_v.shape
    sub = wout_ref.shape[0]
    dk = win_ref.shape[0]
    K1 = 6
    cf, cd = sub // 3, D // N
    F2 = 2 * sub
    n_x = n_tp // 2
    RX = split_rows(R)
    hx, hy = RX // 2, (R - RX) // 2
    t = lax.axis_index("tp")
    y = lax.axis_index("fsdp")
    x, c = lax.div(t, 2), lax.rem(t, 2)
    xr, xl, xf = lax.rem(x + 1, n_x), lax.rem(x + n_x - 1, n_x), lax.rem(x + 2, n_x)
    tr, tl, tf = xr * 2 + c, xl * 2 + c, xf * 2 + c
    tsib = x * 2 + 1 - c
    yp = lax.div(y, 2) * 2 + 1 - lax.rem(y, 2)
    yd = n_y - 1 - y
    yo = n_y - 1 - yp
    pair, other, sib = {"fsdp": yp}, {"fsdp": yd}, {"tp": tsib}
    xnb = ({"tp": tr}, {"tp": tl})

    def remote(src, dst, s, r, dev):
        return pltpu.make_async_remote_copy(
            src_ref=src, dst_ref=dst, send_sem=s, recv_sem=r, device_id=dev, device_id_type=pl.DeviceIdType.MESH
        )

    def cols(k, n):
        return pl.ds(pl.multiple_of(k * n, 128), n)

    def wrows(o):
        return pl.ds(pl.multiple_of(o * dk, 16), dk)

    def sseq(m):
        return lax.rem(m, 2) * 3 + lax.div(m, 2)

    def kseq(m):
        return lax.rem(m + 1, 2) * 3 + lax.div(m, 2)

    def win_cols(first, second, k):
        s = jnp.where(k < 3, first, second) if not isinstance(k, int) else (first if k < 3 else second)
        return pl.ds(pl.multiple_of(s * sub + lax.rem(k, 3) * cf, 128), cf)

    def own_w(k):
        return pltpu.make_async_copy(
            win_ref.at[:, win_cols(y, yd, k)], wb.at[wrows(y), cols(k, cf)], ow_sem.at[k]
        )

    def d_copy(k):
        return remote(
            win_ref.at[:, win_cols(yd, y, k)], wb.at[wrows(y), cols(k, cf)], d_s.at[k], d_r.at[k], other
        )

    def s_copy(k):
        return remote(
            win_ref.at[:, win_cols(yp, yo, k)], wb.at[wrows(y), cols(k, cf)], s_s.at[k], s_r.at[k], pair
        )

    def f_copy(k):
        kk = lax.rem(k + 3, K1)
        return remote(
            wb.at[wrows(yp), cols(k, cf)], wb.at[wrows(yp), cols(kk, cf)], f_s.at[kk], f_r.at[kk], other
        )

    def f_recv(k):
        return remote(wb.at[wrows(yo), cols(k, cf)], wb.at[wrows(yo), cols(k, cf)], f_s.at[k], f_r.at[k], other)

    def wo_copy(j):
        return remote(wout_ref.at[:, cols(j, cd)], gout_ref.at[:, cols(j, cd)], wo_s.at[j], wo_r.at[j], other)

    barrier = pltpu.get_barrier_semaphore()
    for dev in (pair, other, *xnb, sib):
        pl.semaphore_signal(barrier, inc=1, device_id=dev, device_id_type=pl.DeviceIdType.MESH)

    def hid_load(part):
        rows = pl.ds(part * (R // 2), R // 2)
        return pltpu.make_async_copy(hid_ref.at[rows], hid_v.at[rows], hid_sem.at[part])

    for part in range(2):
        hid_load(part).start()
    pl.semaphore_wait(barrier, 5)

    s_copy(0).start()
    for m in range(K1):
        d_copy(((m + 1) % 2) * 3 + m // 2).start()

    TR = 16
    hr = R // 2

    def normalize(part):
        hid_load(part).wait()

        @pl.loop(0, hr // TR)
        def _(i):
            rows = pl.ds(pl.multiple_of(part * hr + i * TR, TR), TR)
            v = hid_v[rows, :].astype(F32)
            cen = v - jnp.mean(v, axis=-1, keepdims=True)
            var = jnp.mean(cen * cen, axis=-1, keepdims=True)
            ub[0, rows, :] = (cen * lax.rsqrt(var + LN_EPS) * scale_ref[...]).astype(BF16)

    def urows(yy, tt, part):
        return u_ref.at[yy, tt, pl.ds(part * hr, hr), :]

    def uown(part):
        return ub.at[0, pl.ds(part * hr, hr), :]

    def u_store(part):
        return pltpu.make_async_copy(uown(part), urows(0, t, part), ust_sem.at[part])

    def u_pair(part):
        return remote(uown(part), urows(1, t, part), uy_s.at[part], uy_r.at[part], pair)

    def u_copy(yy, d, part):
        ref = urows(yy, t, part)
        return remote(uown(part) if yy == 0 else ref, ref, ux_s.at[yy, d, part], ux_r.at[yy, d, part], xnb[d])

    def u_fwd(yy, d):
        ref = urows(yy, (tl, tr)[d], d)
        return remote(ref, ref, uf_s.at[yy, d], uf_r.at[yy, d], xnb[d])

    SIB = ((t, 0), (t, 1), (tl, 0), (tr, 1), (tl, 1), (tr, 0), (tf, 0), (tf, 1))

    def u_sib(yy, i):
        ref = urows(yy, *SIB[i])
        return remote(uown(i) if yy == 0 and i < 2 else ref, ref, ub_s.at[yy, i], ub_r.at[yy, i], sib)

    def u_start(yy):
        for i in range(2):
            u_copy(yy, 0, i).start()
            u_copy(yy, 1, 1 - i).start()

    def u_first(yy):
        u_copy(yy, 0, 0).wait_recv()
        u_fwd(yy, 0).start()
        u_copy(yy, 1, 1).wait_recv()
        u_fwd(yy, 1).start()
        u_sib(yy, 2).start()
        u_sib(yy, 3).start()

    def u_second(yy):
        u_copy(yy, 0, 1).wait_recv()
        u_sib(yy, 4).start()
        u_copy(yy, 1, 0).wait_recv()
        u_sib(yy, 5).start()

    def u_third(yy):
        for d in range(2):
            u_fwd(yy, d).wait_recv()
            u_sib(yy, 6 + d).start()

    normalize(0)
    u_copy(0, 0, 0).start()
    u_pair(0).start()
    normalize(1)
    u_copy(0, 1, 1).start()
    u_copy(0, 0, 1).start()
    u_copy(0, 1, 0).start()
    u_pair(1).start()
    for i in range(2):
        u_sib(0, i).start()
        u_store(i).start()
    for m in range(1, K1):
        s_copy((m % 2) * 3 + m // 2).start()
    for k in range(K1):
        own_w(k).start()

    def block(i):
        yy = lax.div(i, n_tp)
        m = lax.div(lax.rem(i, n_tp), 2)
        off = lax.div(m * (m + 1), 2)
        return yy, lax.rem(x + off, n_x) * 2 + lax.rem(i, 2)

    def up(n, blk, m0, m1, event=None):
        def loads(idx):
            yy, tt = block(blk(idx))
            s = lax.rem(idx, 2)
            return [
                pltpu.make_async_copy(urows(yy, tt, p), ub.at[s, pl.ds(p * hr, hr), :], ld_sem.at[s, p])
                for p in range(2)
            ]

        for cp in loads(0):
            cp.start()

        @pl.loop(0, n)
        def _(idx):
            if event is not None:
                event(idx)

            @pl.when(idx + 1 < n)
            def _():
                for cp in loads(idx + 1):
                    cp.start()

            for cp in loads(idx):
                cp.wait()
            yy, tt = block(blk(idx))
            rows = pl.ds(pl.multiple_of((yy * n_tp + tt) * R, 16), R)

            @pl.loop(m0(idx), m1(idx))
            def _(m):
                k = kseq(m)
                pre = jnp.dot(ub[lax.rem(idx, 2)], wb[:, cols(k, cf)], preferred_element_type=F32)
                h[rows, cols(k, cf)] = jax.nn.gelu(pre, approximate=True).astype(BF16)

    def s_event(m):
        s_copy(sseq(m)).wait_recv()
        f_copy(sseq(m)).start()

    def w_ready(m):
        k = kseq(m)
        d_copy(k).wait_recv()
        f_recv(k).wait_recv()

    s_event(0)
    u_first(0)
    u_second(0)
    for i in range(2):
        u_pair(i).wait_recv()
    u_start(1)
    for i in range(2):
        u_sib(1, i).start()
    s_event(1)
    u_third(0)
    for i in range(8):
        u_sib(0, i).wait_recv()
    for i in range(2):
        u_sib(1, i).wait_recv()
    for k in range(K1):
        own_w(k).wait()

    for i in range(2):
        u_store(i).wait()
        u_pair(i).wait_send()
        u_sib(0, i).wait_send()
        for d in range(2):
            u_copy(0, d, i).wait_send()

    def same(v):
        return lambda idx: v

    def straight(idx):
        return idx

    s_event(2)
    s_event(3)
    w_ready(0)
    w_ready(1)
    up(10, straight, same(0), same(2))
    s_event(4)
    w_ready(2)
    u_first(1)
    up(10, straight, same(2), same(3))
    s_event(5)
    for j in range(SLOTS):
        wo_copy(j).start()
    w_ready(3)
    up(10, straight, same(3), same(4))
    u_second(1)
    w_ready(4)
    for i in range(2, 6):
        u_sib(1, i).wait_recv()

    def early(idx):
        return lax.div(19 - idx, 16)

    def last_event(idx):
        @pl.when(idx == 4)
        def _():
            w_ready(5)

        @pl.when(idx == 11)
        def _():
            u_third(1)

        @pl.when(idx == 17)
        def _():
            for i in range(6, 8):
                u_sib(1, i).wait_recv()

    up(
        20,
        lambda idx: idx - 4 + 14 * early(idx),
        lambda idx: (1 - early(idx)) * (4 + lax.div(idx, 14) - 5 * lax.div(idx, 18)),
        lambda idx: K1 - early(idx),
        last_event,
    )

    for k in range(K1):
        f_copy(k).wait_send()
        d_copy(k).wait_send()
        s_copy(k).wait_send()

    def s2(j):
        return lax.rem(j, 2)

    def s4(j):
        return lax.rem(j, SLOTS)

    def width(j):
        return cd // 2 if isinstance(j, int) and j >= N - 1 else cd

    def dcols(j):
        if width(j) == cd:
            return cols(j, cd)
        return pl.ds((N - 1) * cd + (j - N + 1) * (cd // 2), cd // 2)

    def narrow(j):
        return pl.ds(0, width(j))

    def sib_copy(j):
        w = narrow(j)
        return remote(sibst.at[:, :, :, w], sibr.at[s2(j), :, :, :, w], sb_s, sb_r.at[s2(j)], sib)

    def yey_copy(j):
        w = narrow(j)
        src = own.at[s4(j), 1, :, pl.ds(RX, R - RX), w]
        return remote(src, yey.at[s4(j), :, :, w], yey_s.at[s2(j)], yey_r.at[s4(j)], pair)

    def yex_copy(j):
        w = narrow(j)
        return remote(own.at[s4(j), 1, x, pl.ds(0, RX), w], yex.at[s4(j), :, w], yex_s.at[s2(j)], yex_r.at[s4(j)], pair)

    def fx_copy(j, d):
        w = narrow(j)
        src = own.at[s4(j), :, xf, pl.ds(d * hx, hx), w]
        return remote(src, fx.at[s4(j), d, :, :, w], fx_s.at[s2(j), d], fx_r.at[s4(j), d], xnb[d])

    def nx_copy(j, d):
        w = narrow(j)
        src = own.at[s4(j), :, (xr, xl)[d], pl.ds(0, RX), w]
        return remote(src, nx.at[s4(j), d, :, :, w], nx_s.at[s2(j), d], nx_r.at[s4(j), d], xnb[d])

    def fy_copy(j, d):
        w = narrow(j)
        src = own.at[s4(j), 0, xf, pl.ds(RX + d * hy, hy), w]
        return remote(src, fy.at[s4(j), d, :, w], fy_s.at[s2(j), d], fy_r.at[s4(j), d], xnb[d])

    def ny_copy(j, d):
        w = narrow(j)
        src = own.at[s4(j), 0, (xr, xl)[d], pl.ds(RX, R - RX), w]
        return remote(src, ny.at[s4(j), d, :, w], ny_s.at[s2(j), d], ny_r.at[s4(j), d], xnb[d])

    def out_copy(j):
        return pltpu.make_async_copy(hid_v.at[:, dcols(j)], out_ref.at[:, dcols(j)], out_sem.at[j])

    def when_static(cond, fn):
        if isinstance(cond, bool):
            if cond:
                fn()
        else:
            pl.when(cond)(fn)

    def send(copy, j, *a):
        when_static(j >= 2, lambda: copy(j - 2, *a).wait_send())
        copy(j, *a).start()

    def w2_cols(j):
        return pl.ds(pl.multiple_of(s2(j) * cd, 128), width(j))

    def w2_loads(j):
        lo, hi = pl.ds(0, sub), pl.ds(sub, sub)
        return (
            pltpu.make_async_copy(wout_ref.at[:, dcols(j)], wb.at[lo, w2_cols(j)], w2_sem.at[s2(j), 0]),
            pltpu.make_async_copy(gout_ref.at[:, dcols(j)], wb.at[hi, w2_cols(j)], w2_sem.at[s2(j), 1]),
        )

    def fetch(j):
        if not (isinstance(j, int) and j == N):
            wo_copy(j).wait_recv()
        for cp in w2_loads(j):
            cp.start()

    def down(j):
        W = slice(0, width(j))
        for cp in w2_loads(j):
            cp.wait()

        if isinstance(j, int):
            if j < N:
                fetch(j + 1)
        else:
            pl.when(j + 1 < N - 1)(lambda: fetch(j + 1))
            pl.when(j + 1 == N - 1)(lambda: fetch(N - 1))
        when_static(j >= 1, lambda: sib_copy(j - 1).wait_send())

        def part(i, cc):
            yy, xx = lax.div(i, n_x), lax.rem(i, n_x)
            rows = pl.ds(pl.multiple_of((yy * n_tp + xx * 2 + cc) * R, 16), R)
            return jnp.dot(h[rows, :], wb[:F2, w2_cols(j)], preferred_element_type=F32)

        @pl.loop(0, 2 * n_x)
        def _(i):
            sibst[lax.div(i, n_x), lax.rem(i, n_x), :, W] = part(i, 1 - c)

        sib_copy(j).start()

        @pl.loop(0, 2 * n_x)
        def _(i):
            own[s4(j), lax.div(i, n_x), lax.rem(i, n_x), :, W] = part(i, c)

    def stage1(j):
        W = slice(0, width(j))
        sib_copy(j).wait_recv()

        @pl.loop(0, 2 * n_x)
        def _(i):
            yy, xx = lax.div(i, n_x), lax.rem(i, n_x)
            own[s4(j), yy, xx, :, W] = own[s4(j), yy, xx, :, W] + sibr[s2(j), yy, xx, :, W]

        send(yey_copy, j)
        for d in range(2):
            send(fx_copy, j, d)

    def stage2(j):
        s, W = s4(j), slice(0, width(j))
        for d in range(2):
            fx_copy(j, d).wait_recv()
            b, rows = (xr, xl)[d], slice(d * hx, (d + 1) * hx)
            for yy in range(2):
                own[s, yy, b, rows, W] = own[s, yy, b, rows, W] + fx[s, d, yy, :, W]
        for d in range(2):
            send(nx_copy, j, d)
        yey_copy(j).wait_recv()

        @pl.loop(0, n_x)
        def _(i):
            own[s, 0, i, RX:, W] = own[s, 0, i, RX:, W] + yey[s, i, :, W]

        for d in range(2):
            send(fy_copy, j, d)

    def stage3(j):
        s, W = s4(j), slice(0, width(j))
        for d in range(2):
            fy_copy(j, d).wait_recv()
            b, rows = (xr, xl)[d], slice(RX + d * hy, RX + (d + 1) * hy)
            own[s, 0, b, rows, W] = own[s, 0, b, rows, W] + fy[s, d, :, W]
        for d in range(2):
            ny_copy(j, d).start()
        for d in range(2):
            nx_copy(j, d).wait_recv()
        for yy in (1, 0):
            own[s, yy, x, :RX, W] = own[s, yy, x, :RX, W] + nx[s, 0, yy, :, W] + nx[s, 1, yy, :, W]
        yex_copy(j).start()

    def stage4(j):
        s, W = s4(j), slice(0, width(j))
        for d in range(2):
            ny_copy(j, d).wait_recv()
        lo = own[s, 0, x, RX:, W] + ny[s, 0, :, W] + ny[s, 1, :, W]
        hid_v[RX:, dcols(j)] = (hid_v[RX:, dcols(j)].astype(F32) + lo).astype(BF16)
        yex_copy(j).wait_recv()
        hi = own[s, 0, x, :RX, W] + yex[s, :, W]
        hid_v[:RX, dcols(j)] = (hid_v[:RX, dcols(j)].astype(F32) + hi).astype(BF16)
        out_copy(j).start()
        yex_copy(j).wait_send()
        for d in range(2):
            ny_copy(j, d).wait_send()

    fetch(0)

    @pl.loop(0, N - 1)
    def _(j):
        @pl.when(j + SLOTS < N)
        def _():
            wo_copy(j + SLOTS).start()

        down(j)
        stage1(j)
        pl.when(j >= 1)(lambda: stage2(j - 1))
        pl.when(j >= 2)(lambda: stage3(j - 2))
        pl.when(j >= 3)(lambda: stage4(j - 3))

    for j in range(N - 1, N + 4):
        if j <= N:
            down(j)
            stage1(j)
        for lag, stage in ((1, stage2), (2, stage3), (3, stage4)):
            if j - lag <= N:
                stage(j - lag)

    for yy in range(2):
        for d in range(2):
            u_fwd(yy, d).wait_send()
            if yy == 1:
                for part in range(2):
                    u_copy(yy, d, part).wait_send()
        for i in range(2 * (1 - yy), 8):
            u_sib(yy, i).wait_send()
    sib_copy(N).wait_send()
    for j in (N - 1, N):
        yey_copy(j).wait_send()
        for d in range(2):
            for copy in (fx_copy, nx_copy, fy_copy):
                copy(j, d).wait_send()

    @pl.loop(0, N)
    def _(j):
        wo_copy(j).wait_send()

    @pl.loop(0, N - 1)
    def _(j):
        out_copy(j).wait()

    for j in (N - 1, N):
        out_copy(j).wait()


def make_local(n_tp, n_y, N):
    def local_mlp(hidden, ln_scale, w_in, w_out):
        R, D = hidden.shape
        sub = w_out.shape[0]
        cd = D // N
        n_x = n_tp // 2
        RX = split_rows(R)
        any_spec = pl.BlockSpec(memory_space=pl.ANY)
        dma = pltpu.SemaphoreType.DMA
        vm = pltpu.VMEM
        S = SLOTS
        out, _, _ = pl.pallas_call(
            functools.partial(mlp_kernel, n_tp, n_y, N),
            out_shape=(
                jax.ShapeDtypeStruct((R, D), BF16),
                jax.ShapeDtypeStruct((2, n_tp, R, D), BF16),
                jax.ShapeDtypeStruct((sub, D), BF16),
            ),
            in_specs=[any_spec, pl.BlockSpec(memory_space=vm), any_spec, any_spec],
            out_specs=(any_spec, any_spec, any_spec),
            scratch_shapes=[
                vm((D, 2 * sub), BF16),
                vm((2 * n_tp * R, 2 * sub), BF16),
                vm((2, R, D), BF16),
                vm((R, D), BF16),
                vm((S, 2, n_x, R, cd), F32),
                vm((2, n_x, R, cd), F32),
                vm((2, 2, n_x, R, cd), F32),
                vm((S, n_x, R - RX, cd), F32),
                vm((S, 2, 2, RX // 2, cd), F32),
                vm((S, 2, 2, RX, cd), F32),
                vm((S, 2, (R - RX) // 2, cd), F32),
                vm((S, 2, R - RX, cd), F32),
                vm((S, RX, cd), F32),
                dma((2,)), dma((2,)), dma((2, 2)), dma((6,)), dma((2, 2)), dma((N + 1,)),
                dma((6,)), dma((6,)), dma((6,)), dma((6,)), dma((6,)), dma((6,)), dma((N,)), dma((N,)),
                dma((2,)), dma((2,)), dma((2, 2, 2)), dma((2, 2, 2)), dma((2, 2)), dma((2, 2)), dma((2, 8)), dma((2, 8)),
                dma, dma((2,)), dma((2,)), dma((S,)), dma((2, 2)), dma((S, 2)), dma((2, 2)), dma((S, 2)),
                dma((2, 2)), dma((S, 2)), dma((2, 2)), dma((S, 2)), dma((2,)), dma((S,)),
            ],
            compiler_params=pltpu.CompilerParams(
                collective_id=0, has_side_effects=True, vmem_limit_bytes=67043328
            ),
            cost_estimate=pl.CostEstimate(
                flops=4 * n_tp * R * D * w_in.shape[1], bytes_accessed=8 * D * w_in.shape[1], transcendentals=0
            ),
            name="mlp",
        )(hidden, ln_scale.reshape(1, D), w_in, w_out)
        return out

    return local_mlp


def solution(mesh):
    return jax.shard_map(
        make_local(mesh.shape["tp"], mesh.shape["fsdp"], CHUNKS),
        mesh=mesh,
        in_specs=(P(("data", "fsdp", "tp"), None), P(None), P("fsdp", "tp"), P(("tp", "fsdp"), None)),
        out_specs=P(("data", "fsdp", "tp"), None),
        check_vma=False,
    )
```

```python
import functools

import jax
import jax.numpy as jnp
from jax import lax
from jax.experimental import pallas as pl
from jax.experimental.pallas import tpu as pltpu
from jax.sharding import PartitionSpec as P

LN_EPS = 1e-6
CHUNKS = 24
F32 = jnp.float32
BF16 = jnp.bfloat16
SLOTS = 4


def split_rows(R):
    return R * 9 // 16 // 16 * 16


def mlp_kernel(
    n_tp, n_y, N, hid_ref, scale_ref, win_ref, wout_ref, out_ref, u_ref, gout_ref,
    wb, h, w2b, ub, hid_v, own, sibst, sibr, yey, fx, nx, fy, ny, yex,
    hid_sem, ust_sem, ld_sem, ow_sem, w2_sem, out_sem,
    d_s, d_r, s_s, s_r, f_s, f_r, wo_s, wo_r,
    uy_s, uy_r, ux_s, ux_r, uf_s, uf_r, ub_s, ub_r,
    sb_s, sb_r, yey_s, yey_r, fx_s, fx_r, nx_s, nx_r, fy_s, fy_r, ny_s, ny_r, yex_s, yex_r,
):
    R, D = hid_v.shape
    sub = wout_ref.shape[0]
    dk = win_ref.shape[0]
    K1 = 6
    cf, cd = sub // 3, D // N
    n_x = n_tp // 2
    RX = split_rows(R)
    hx, hy = RX // 2, (R - RX) // 2
    t = lax.axis_index("tp")
    y = lax.axis_index("fsdp")
    x, c = lax.div(t, 2), lax.rem(t, 2)
    xr, xl, xf = lax.rem(x + 1, n_x), lax.rem(x + n_x - 1, n_x), lax.rem(x + 2, n_x)
    tr, tl, tf = xr * 2 + c, xl * 2 + c, xf * 2 + c
    tsib = x * 2 + 1 - c
    yp = lax.div(y, 2) * 2 + 1 - lax.rem(y, 2)
    yd = n_y - 1 - y
    yo = n_y - 1 - yp
    pair, other, sib = {"fsdp": yp}, {"fsdp": yd}, {"tp": tsib}
    xnb = ({"tp": tr}, {"tp": tl})

    def remote(src, dst, s, r, dev):
        return pltpu.make_async_remote_copy(
            src_ref=src, dst_ref=dst, send_sem=s, recv_sem=r, device_id=dev, device_id_type=pl.DeviceIdType.MESH
        )

    def cols(k, n):
        return pl.ds(pl.multiple_of(k * n, 128), n)

    def wrows(o):
        return pl.ds(pl.multiple_of(o * dk, 16), dk)

    def sseq(m):
        return lax.rem(m, 2) * 3 + lax.div(m, 2)

    def kseq(m):
        return lax.rem(m + 1, 2) * 3 + lax.div(m, 2)

    def win_cols(first, second, k):
        s = jnp.where(k < 3, first, second) if not isinstance(k, int) else (first if k < 3 else second)
        return pl.ds(pl.multiple_of(s * sub + lax.rem(k, 3) * cf, 128), cf)

    def own_w(k):
        return pltpu.make_async_copy(
            win_ref.at[:, win_cols(y, yd, k)], wb.at[wrows(y), cols(k, cf)], ow_sem.at[k]
        )

    def d_copy(k):
        return remote(
            win_ref.at[:, win_cols(yd, y, k)], wb.at[wrows(y), cols(k, cf)], d_s.at[k], d_r.at[k], other
        )

    def s_copy(k):
        return remote(
            win_ref.at[:, win_cols(yp, yo, k)], wb.at[wrows(y), cols(k, cf)], s_s.at[k], s_r.at[k], pair
        )

    def f_copy(k):
        kk = lax.rem(k + 3, K1)
        return remote(
            wb.at[wrows(yp), cols(k, cf)], wb.at[wrows(yp), cols(kk, cf)], f_s.at[kk], f_r.at[kk], other
        )

    def f_recv(k):
        return remote(wb.at[wrows(yo), cols(k, cf)], wb.at[wrows(yo), cols(k, cf)], f_s.at[k], f_r.at[k], other)

    def wo_copy(j):
        return remote(wout_ref.at[:, cols(j, cd)], gout_ref.at[:, cols(j, cd)], wo_s.at[j], wo_r.at[j], other)

    def s2(j):
        return lax.rem(j, 2)

    def s4(j):
        return lax.rem(j, SLOTS)

    def width(j):
        return cd // 2 if isinstance(j, int) and j >= N - 1 else cd

    def dcols(j):
        if width(j) == cd:
            return cols(j, cd)
        return pl.ds((N - 1) * cd + (j - N + 1) * (cd // 2), cd // 2)

    def narrow(j):
        return pl.ds(0, width(j))

    def w2_loads(j):
        lo, hi, w = pl.ds(0, sub), pl.ds(sub, sub), narrow(j)
        return (
            pltpu.make_async_copy(wout_ref.at[:, dcols(j)], w2b.at[s2(j), lo, w], w2_sem.at[s2(j), 0]),
            pltpu.make_async_copy(gout_ref.at[:, dcols(j)], w2b.at[s2(j), hi, w], w2_sem.at[s2(j), 1]),
        )

    def fetch(j):
        if not (isinstance(j, int) and j == N):
            wo_copy(j).wait_recv()
        for cp in w2_loads(j):
            cp.start()

    barrier = pltpu.get_barrier_semaphore()
    for dev in (pair, other, *xnb, sib):
        pl.semaphore_signal(barrier, inc=1, device_id=dev, device_id_type=pl.DeviceIdType.MESH)

    def hid_load(part):
        rows = pl.ds(part * (R // 2), R // 2)
        return pltpu.make_async_copy(hid_ref.at[rows], hid_v.at[rows], hid_sem.at[part])

    for part in range(2):
        hid_load(part).start()
    pl.semaphore_wait(barrier, 5)

    s_copy(0).start()
    for m in range(K1):
        d_copy(((m + 1) % 2) * 3 + m // 2).start()

    TR = 16
    hr = R // 2

    def normalize(part):
        hid_load(part).wait()

        @pl.loop(0, hr // TR)
        def _(i):
            rows = pl.ds(pl.multiple_of(part * hr + i * TR, TR), TR)
            v = hid_v[rows, :].astype(F32)
            cen = v - jnp.mean(v, axis=-1, keepdims=True)
            var = jnp.mean(cen * cen, axis=-1, keepdims=True)
            ub[0, rows, :] = (cen * lax.rsqrt(var + LN_EPS) * scale_ref[...]).astype(BF16)

    def urows(yy, tt, part):
        return u_ref.at[yy, tt, pl.ds(part * hr, hr), :]

    def uown(part):
        return ub.at[0, pl.ds(part * hr, hr), :]

    def u_store(part):
        return pltpu.make_async_copy(uown(part), urows(0, t, part), ust_sem.at[part])

    def u_pair(part):
        return remote(uown(part), urows(1, t, part), uy_s.at[part], uy_r.at[part], pair)

    def u_copy(yy, d, part):
        ref = urows(yy, t, part)
        return remote(uown(part) if yy == 0 else ref, ref, ux_s.at[yy, d, part], ux_r.at[yy, d, part], xnb[d])

    def u_fwd(yy, d):
        ref = urows(yy, (tl, tr)[d], d)
        return remote(ref, ref, uf_s.at[yy, d], uf_r.at[yy, d], xnb[d])

    SIB = ((t, 0), (t, 1), (tl, 0), (tr, 0), (tl, 1), (tr, 1), (tf, 0), (tf, 1))

    def u_sib(yy, i):
        ref = urows(yy, *SIB[i])
        return remote(uown(i) if yy == 0 and i < 2 else ref, ref, ub_s.at[yy, i], ub_r.at[yy, i], sib)

    def u_start(yy, part):
        for d in range(2):
            u_copy(yy, d, part).start()

    def u_near(yy, part):
        for d in range(2):
            u_copy(yy, d, part).wait_recv()
            u_sib(yy, 2 + 2 * part + d).start()

    def u_far(yy):
        for d in range(2):
            u_fwd(yy, d).wait_recv()
            u_sib(yy, 6 + d).start()

    for part in range(2):
        normalize(part)
        u_start(0, part)
        u_pair(part).start()
    for i in range(2):
        u_sib(0, i).start()
        u_store(i).start()
    for m in range(1, K1):
        s_copy((m % 2) * 3 + m // 2).start()
    for k in range(K1):
        own_w(k).start()

    def block(q):
        e, g = lax.div(q, 12), lax.div(q, 14)
        i = q + 2 * lax.div(q, 6) * (1 - e) - 6 * (e - g)
        yy = lax.div(i, n_tp)
        m = lax.div(lax.rem(i, n_tp), 2)
        off = lax.div(m * (m + 1), 2)
        return yy, lax.rem(x + off, n_x) * 2 + lax.rem(i, 2)

    def up(n, blk, m0, m1, event=None):
        def loads(idx):
            yy, tt = block(blk(idx))
            s = lax.rem(idx, 2)
            return [
                pltpu.make_async_copy(urows(yy, tt, p), ub.at[s, pl.ds(p * hr, hr), :], ld_sem.at[s, p])
                for p in range(2)
            ]

        for cp in loads(0):
            cp.start()

        @pl.loop(0, n)
        def _(idx):
            if event is not None:
                event(idx)

            @pl.when(idx + 1 < n)
            def _():
                for cp in loads(idx + 1):
                    cp.start()

            for cp in loads(idx):
                cp.wait()
            yy, tt = block(blk(idx))
            rows = pl.ds(pl.multiple_of((yy * n_tp + tt) * R, 16), R)

            @pl.loop(m0(idx), m1(idx))
            def _(m):
                k = kseq(m)
                pre = jnp.dot(ub[lax.rem(idx, 2)], wb[:, cols(k, cf)], preferred_element_type=F32)
                h[rows, cols(k, cf)] = jax.nn.gelu(pre, approximate=True).astype(BF16)

    def s_event(m):
        s_copy(sseq(m)).wait_recv()
        f_copy(sseq(m)).start()

    def w_ready(m):
        k = kseq(m)
        d_copy(k).wait_recv()
        f_recv(k).wait_recv()

    def same(v):
        return lambda idx: v

    def straight(idx):
        return idx

    s_event(0)
    u_near(0, 0)
    u_pair(0).wait_recv()
    u_start(1, 0)
    u_sib(1, 0).start()
    u_near(0, 1)
    u_pair(1).wait_recv()
    u_start(1, 1)
    for d in range(2):
        u_fwd(0, d).start()
    u_sib(1, 1).start()
    s_event(1)
    u_near(1, 0)
    s_event(2)
    for i in range(6):
        u_sib(0, i).wait_recv()
    for i in range(2):
        u_sib(1, i).wait_recv()
    for k in range(K1):
        own_w(k).wait()
    for i in range(2):
        u_store(i).wait()
        u_pair(i).wait_send()
        u_sib(0, i).wait_send()
        for d in range(2):
            u_copy(0, d, i).wait_send()

    w_ready(0)
    up(8, straight, same(0), same(1))
    s_event(3)
    w_ready(1)
    up(8, straight, same(1), same(2))
    u_near(1, 1)
    for d in range(2):
        u_fwd(1, d).start()
    s_event(4)
    w_ready(2)
    for i in range(2, 6):
        u_sib(1, i).wait_recv()

    def first4(idx):
        return lax.div(15 - idx, 12)

    up(12, lambda idx: idx - 4 + 12 * first4(idx), lambda idx: 2 * (1 - first4(idx)), same(3))
    s_event(5)
    for j in range(SLOTS):
        wo_copy(j).start()
    w_ready(3)
    u_far(0)
    up(12, straight, same(3), same(4))
    w_ready(4)
    for i in range(6, 8):
        u_sib(0, i).wait_recv()

    def first2(idx):
        return lax.div(25 - idx, 24)

    def last_block(idx):
        g = lax.div(idx, 20)
        return idx - 2 + 14 * first2(idx) - 12 * (lax.div(idx, 14) - g) - 6 * g

    def last_event(idx):
        @pl.when(idx == 8)
        def _():
            w_ready(5)

        @pl.when(idx == 12)
        def _():
            u_far(1)

        @pl.when(idx == 15)
        def _():
            fetch(0)

        @pl.when(idx == 21)
        def _():
            for i in range(6, 8):
                u_sib(1, i).wait_recv()

    up(
        24,
        last_block,
        lambda idx: (1 - first2(idx)) * (4 + lax.div(idx, 14)) - 5 * lax.div(idx, 22),
        lambda idx: 5 + lax.div(idx + 16, 24),
        last_event,
    )

    for k in range(K1):
        f_copy(k).wait_send()
        d_copy(k).wait_send()
        s_copy(k).wait_send()

    def sib_copy(j):
        w = narrow(j)
        return remote(sibst.at[:, :, :, w], sibr.at[s2(j), :, :, :, w], sb_s, sb_r.at[s2(j)], sib)

    def yey_copy(j):
        w = narrow(j)
        src = own.at[s4(j), 1, :, pl.ds(RX, R - RX), w]
        return remote(src, yey.at[s4(j), :, :, w], yey_s.at[s2(j)], yey_r.at[s4(j)], pair)

    def yex_copy(j):
        w = narrow(j)
        return remote(own.at[s4(j), 1, x, pl.ds(0, RX), w], yex.at[s4(j), :, w], yex_s.at[s2(j)], yex_r.at[s4(j)], pair)

    def fx_copy(j, d):
        w = narrow(j)
        src = own.at[s4(j), :, xf, pl.ds(d * hx, hx), w]
        return remote(src, fx.at[s4(j), d, :, :, w], fx_s.at[s2(j), d], fx_r.at[s4(j), d], xnb[d])

    def nx_copy(j, d):
        w = narrow(j)
        src = own.at[s4(j), :, (xr, xl)[d], pl.ds(0, RX), w]
        return remote(src, nx.at[s4(j), d, :, :, w], nx_s.at[s2(j), d], nx_r.at[s4(j), d], xnb[d])

    def fy_copy(j, d):
        w = narrow(j)
        src = own.at[s4(j), 0, xf, pl.ds(RX + d * hy, hy), w]
        return remote(src, fy.at[s4(j), d, :, w], fy_s.at[s2(j), d], fy_r.at[s4(j), d], xnb[d])

    def ny_copy(j, d):
        w = narrow(j)
        src = own.at[s4(j), 0, (xr, xl)[d], pl.ds(RX, R - RX), w]
        return remote(src, ny.at[s4(j), d, :, w], ny_s.at[s2(j), d], ny_r.at[s4(j), d], xnb[d])

    def out_copy(j):
        return pltpu.make_async_copy(hid_v.at[:, dcols(j)], out_ref.at[:, dcols(j)], out_sem.at[j])

    def when_static(cond, fn):
        if isinstance(cond, bool):
            if cond:
                fn()
        else:
            pl.when(cond)(fn)

    def send(copy, j, *a):
        when_static(j >= 2, lambda: copy(j - 2, *a).wait_send())
        copy(j, *a).start()

    def down(j):
        W = slice(0, width(j))
        for cp in w2_loads(j):
            cp.wait()

        if isinstance(j, int):
            if j < N:
                fetch(j + 1)
        else:
            pl.when(j + 1 < N - 1)(lambda: fetch(j + 1))
            pl.when(j + 1 == N - 1)(lambda: fetch(N - 1))
        when_static(j >= 1, lambda: sib_copy(j - 1).wait_send())

        def part(i, cc):
            yy, xx = lax.div(i, n_x), lax.rem(i, n_x)
            rows = pl.ds(pl.multiple_of((yy * n_tp + xx * 2 + cc) * R, 16), R)
            return jnp.dot(h[rows, :], w2b[s2(j), :, W], preferred_element_type=F32)

        @pl.loop(0, 2 * n_x)
        def _(i):
            sibst[lax.div(i, n_x), lax.rem(i, n_x), :, W] = part(i, 1 - c)

        sib_copy(j).start()

        @pl.loop(0, 2 * n_x)
        def _(i):
            own[s4(j), lax.div(i, n_x), lax.rem(i, n_x), :, W] = part(i, c)

    def stage1(j):
        W = slice(0, width(j))
        sib_copy(j).wait_recv()

        @pl.loop(0, 2 * n_x)
        def _(i):
            yy, xx = lax.div(i, n_x), lax.rem(i, n_x)
            own[s4(j), yy, xx, :, W] = own[s4(j), yy, xx, :, W] + sibr[s2(j), yy, xx, :, W]

        send(yey_copy, j)
        for d in range(2):
            send(fx_copy, j, d)

    def stage2(j):
        s, W = s4(j), slice(0, width(j))
        for d in range(2):
            fx_copy(j, d).wait_recv()
            b, rows = (xr, xl)[d], slice(d * hx, (d + 1) * hx)
            for yy in range(2):
                own[s, yy, b, rows, W] = own[s, yy, b, rows, W] + fx[s, d, yy, :, W]
        for d in range(2):
            send(nx_copy, j, d)
        yey_copy(j).wait_recv()

        @pl.loop(0, n_x)
        def _(i):
            own[s, 0, i, RX:, W] = own[s, 0, i, RX:, W] + yey[s, i, :, W]

        for d in range(2):
            send(fy_copy, j, d)

    def stage3(j):
        s, W = s4(j), slice(0, width(j))
        for d in range(2):
            fy_copy(j, d).wait_recv()
            b, rows = (xr, xl)[d], slice(RX + d * hy, RX + (d + 1) * hy)
            own[s, 0, b, rows, W] = own[s, 0, b, rows, W] + fy[s, d, :, W]
        for d in range(2):
            ny_copy(j, d).start()
        for d in range(2):
            nx_copy(j, d).wait_recv()
        for yy in (1, 0):
            own[s, yy, x, :RX, W] = own[s, yy, x, :RX, W] + nx[s, 0, yy, :, W] + nx[s, 1, yy, :, W]
        yex_copy(j).start()

    def stage4(j):
        s, W = s4(j), slice(0, width(j))
        for d in range(2):
            ny_copy(j, d).wait_recv()
        lo = own[s, 0, x, RX:, W] + ny[s, 0, :, W] + ny[s, 1, :, W]
        hid_v[RX:, dcols(j)] = (hid_v[RX:, dcols(j)].astype(F32) + lo).astype(BF16)
        yex_copy(j).wait_recv()
        hi = own[s, 0, x, :RX, W] + yex[s, :, W]
        hid_v[:RX, dcols(j)] = (hid_v[:RX, dcols(j)].astype(F32) + hi).astype(BF16)
        out_copy(j).start()
        yex_copy(j).wait_send()
        for d in range(2):
            ny_copy(j, d).wait_send()

    @pl.loop(0, N - 1)
    def _(j):
        @pl.when(j + SLOTS < N)
        def _():
            wo_copy(j + SLOTS).start()

        down(j)
        stage1(j)
        pl.when(j >= 1)(lambda: stage2(j - 1))
        pl.when(j >= 2)(lambda: stage3(j - 2))
        pl.when(j >= 3)(lambda: stage4(j - 3))

    for j in range(N - 1, N + 4):
        if j <= N:
            down(j)
            stage1(j)
        for lag, stage in ((1, stage2), (2, stage3), (3, stage4)):
            if j - lag <= N:
                stage(j - lag)

    for yy in range(2):
        for d in range(2):
            u_fwd(yy, d).wait_send()
            if yy == 1:
                for part in range(2):
                    u_copy(yy, d, part).wait_send()
        for i in range(2 * (1 - yy), 8):
            u_sib(yy, i).wait_send()
    sib_copy(N).wait_send()
    for j in (N - 1, N):
        yey_copy(j).wait_send()
        for d in range(2):
            for copy in (fx_copy, nx_copy, fy_copy):
                copy(j, d).wait_send()

    @pl.loop(0, N)
    def _(j):
        wo_copy(j).wait_send()

    @pl.loop(0, N - 1)
    def _(j):
        out_copy(j).wait()

    for j in (N - 1, N):
        out_copy(j).wait()


def make_local(n_tp, n_y, N):
    def local_mlp(hidden, ln_scale, w_in, w_out):
        R, D = hidden.shape
        sub = w_out.shape[0]
        cd = D // N
        n_x = n_tp // 2
        RX = split_rows(R)
        any_spec = pl.BlockSpec(memory_space=pl.ANY)
        dma = pltpu.SemaphoreType.DMA
        vm = pltpu.VMEM
        S = SLOTS
        out, _, _ = pl.pallas_call(
            functools.partial(mlp_kernel, n_tp, n_y, N),
            out_shape=(
                jax.ShapeDtypeStruct((R, D), BF16),
                jax.ShapeDtypeStruct((2, n_tp, R, D), BF16),
                jax.ShapeDtypeStruct((sub, D), BF16),
            ),
            in_specs=[any_spec, pl.BlockSpec(memory_space=vm), any_spec, any_spec],
            out_specs=(any_spec, any_spec, any_spec),
            scratch_shapes=[
                vm((D, 2 * sub), BF16),
                vm((2 * n_tp * R, 2 * sub), BF16),
                vm((2, 2 * sub, cd), BF16),
                vm((2, R, D), BF16),
                vm((R, D), BF16),
                vm((S, 2, n_x, R, cd), F32),
                vm((2, n_x, R, cd), F32),
                vm((2, 2, n_x, R, cd), F32),
                vm((S, n_x, R - RX, cd), F32),
                vm((S, 2, 2, RX // 2, cd), F32),
                vm((S, 2, 2, RX, cd), F32),
                vm((S, 2, (R - RX) // 2, cd), F32),
                vm((S, 2, R - RX, cd), F32),
                vm((S, RX, cd), F32),
                dma((2,)), dma((2,)), dma((2, 2)), dma((6,)), dma((2, 2)), dma((N + 1,)),
                dma((6,)), dma((6,)), dma((6,)), dma((6,)), dma((6,)), dma((6,)), dma((N,)), dma((N,)),
                dma((2,)), dma((2,)), dma((2, 2, 2)), dma((2, 2, 2)), dma((2, 2)), dma((2, 2)), dma((2, 8)), dma((2, 8)),
                dma, dma((2,)), dma((2,)), dma((S,)), dma((2, 2)), dma((S, 2)), dma((2, 2)), dma((S, 2)),
                dma((2, 2)), dma((S, 2)), dma((2, 2)), dma((S, 2)), dma((2,)), dma((S,)),
            ],
            compiler_params=pltpu.CompilerParams(
                collective_id=0, has_side_effects=True, vmem_limit_bytes=67043328
            ),
            cost_estimate=pl.CostEstimate(
                flops=4 * n_tp * R * D * w_in.shape[1], bytes_accessed=8 * D * w_in.shape[1], transcendentals=0
            ),
            name="mlp",
        )(hidden, ln_scale.reshape(1, D), w_in, w_out)
        return out

    return local_mlp


def solution(mesh):
    return jax.shard_map(
        make_local(mesh.shape["tp"], mesh.shape["fsdp"], CHUNKS),
        mesh=mesh,
        in_specs=(P(("data", "fsdp", "tp"), None), P(None), P("fsdp", "tp"), P(("tp", "fsdp"), None)),
        out_specs=P(("data", "fsdp", "tp"), None),
        check_vma=False,
    )
```

```python
import functools

import jax
import jax.numpy as jnp
from jax import lax
from jax.experimental import pallas as pl
from jax.experimental.pallas import tpu as pltpu
from jax.sharding import PartitionSpec as P

LN_EPS = 1e-6
CHUNKS = 24
F32 = jnp.float32
BF16 = jnp.bfloat16
SLOTS = 4


def split_rows(R):
    return R * 9 // 16 // 16 * 16


def mlp_kernel(
    n_tp, n_y, N, hid_ref, scale_ref, win_ref, wout_ref, out_ref, u_ref, gout_ref,
    wb, h, w2b, ub, hid_v, own, sibst, sibr, yey, fx, nx, fy, ny, yex,
    hid_sem, ust_sem, ld_sem, ow_sem, w2_sem, out_sem,
    d_s, d_r, s_s, s_r, f_s, f_r, wo_s, wo_r,
    uy_s, uy_r, ux_s, ux_r, uf_s, uf_r, ub_s, ub_r,
    sb_s, sb_r, yey_s, yey_r, fx_s, fx_r, nx_s, nx_r, fy_s, fy_r, ny_s, ny_r, yex_s, yex_r,
):
    R, D = hid_v.shape
    sub = wout_ref.shape[0]
    dk = win_ref.shape[0]
    K1 = 6
    cf, cd = sub // 3, D // N
    n_x = n_tp // 2
    RX = split_rows(R)
    hx, hy = RX // 2, (R - RX) // 2
    t = lax.axis_index("tp")
    y = lax.axis_index("fsdp")
    x, c = lax.div(t, 2), lax.rem(t, 2)
    xr, xl, xf = lax.rem(x + 1, n_x), lax.rem(x + n_x - 1, n_x), lax.rem(x + 2, n_x)
    tr, tl, tf = xr * 2 + c, xl * 2 + c, xf * 2 + c
    tsib = x * 2 + 1 - c
    yp = lax.div(y, 2) * 2 + 1 - lax.rem(y, 2)
    yd = n_y - 1 - y
    yo = n_y - 1 - yp
    pair, other, sib = {"fsdp": yp}, {"fsdp": yd}, {"tp": tsib}
    xnb = ({"tp": tr}, {"tp": tl})

    def remote(src, dst, s, r, dev):
        return pltpu.make_async_remote_copy(
            src_ref=src, dst_ref=dst, send_sem=s, recv_sem=r, device_id=dev, device_id_type=pl.DeviceIdType.MESH
        )

    def cols(k, n):
        return pl.ds(pl.multiple_of(k * n, 128), n)

    def wrows(o):
        return pl.ds(pl.multiple_of(o * dk, 16), dk)

    def sseq(m):
        return lax.rem(m, 2) * 3 + lax.div(m, 2)

    def kseq(m):
        return lax.rem(m + 1, 2) * 3 + lax.div(m, 2)

    def win_cols(first, second, k):
        s = jnp.where(k < 3, first, second) if not isinstance(k, int) else (first if k < 3 else second)
        return pl.ds(pl.multiple_of(s * sub + lax.rem(k, 3) * cf, 128), cf)

    def own_w(k):
        return pltpu.make_async_copy(
            win_ref.at[:, win_cols(y, yd, k)], wb.at[k, wrows(y)], ow_sem.at[k]
        )

    def d_copy(k):
        return remote(
            win_ref.at[:, win_cols(yd, y, k)], wb.at[k, wrows(y)], d_s.at[k], d_r.at[k], other
        )

    def s_copy(k):
        return remote(
            win_ref.at[:, win_cols(yp, yo, k)], wb.at[k, wrows(y)], s_s.at[k], s_r.at[k], pair
        )

    def f_copy(k):
        kk = lax.rem(k + 3, K1)
        return remote(
            wb.at[k, wrows(yp)], wb.at[kk, wrows(yp)], f_s.at[kk], f_r.at[kk], other
        )

    def f_recv(k):
        return remote(wb.at[k, wrows(yo)], wb.at[k, wrows(yo)], f_s.at[k], f_r.at[k], other)

    def wo_copy(j):
        return remote(wout_ref.at[:, cols(j, cd)], gout_ref.at[:, cols(j, cd)], wo_s.at[j], wo_r.at[j], other)

    def s2(j):
        return lax.rem(j, 2)

    def s4(j):
        return lax.rem(j, SLOTS)

    def width(j):
        return cd // 2 if isinstance(j, int) and j >= N - 1 else cd

    def dcols(j):
        if width(j) == cd:
            return cols(j, cd)
        return pl.ds((N - 1) * cd + (j - N + 1) * (cd // 2), cd // 2)

    def narrow(j):
        return pl.ds(0, width(j))

    def w2_loads(j):
        lo, hi, w = pl.ds(0, sub), pl.ds(sub, sub), narrow(j)
        return (
            pltpu.make_async_copy(wout_ref.at[:, dcols(j)], w2b.at[s2(j), lo, w], w2_sem.at[s2(j), 0]),
            pltpu.make_async_copy(gout_ref.at[:, dcols(j)], w2b.at[s2(j), hi, w], w2_sem.at[s2(j), 1]),
        )

    def fetch(j):
        if not (isinstance(j, int) and j == N):
            wo_copy(j).wait_recv()
        for cp in w2_loads(j):
            cp.start()

    barrier = pltpu.get_barrier_semaphore()
    for dev in (pair, other, *xnb, sib):
        pl.semaphore_signal(barrier, inc=1, device_id=dev, device_id_type=pl.DeviceIdType.MESH)

    def hid_load(part):
        rows = pl.ds(part * (R // 2), R // 2)
        return pltpu.make_async_copy(hid_ref.at[rows], hid_v.at[rows], hid_sem.at[part])

    for part in range(2):
        hid_load(part).start()
    pl.semaphore_wait(barrier, 5)

    s_copy(0).start()
    for m in range(K1):
        d_copy(((m + 1) % 2) * 3 + m // 2).start()

    TR = 16
    hr = R // 2
    lr = max(R // 4, 16)

    def normalize(part):
        hid_load(part).wait()

        @pl.loop(0, hr // TR)
        def _(i):
            rows = pl.ds(pl.multiple_of(part * hr + i * TR, TR), TR)
            v = hid_v[rows, :].astype(F32)
            cen = v - jnp.mean(v, axis=-1, keepdims=True)
            var = jnp.mean(cen * cen, axis=-1, keepdims=True)
            ub[0, rows, :] = (cen * lax.rsqrt(var + LN_EPS) * scale_ref[...]).astype(BF16)

    def urows(yy, tt, part):
        return u_ref.at[yy, tt, pl.ds(part * hr, hr), :]

    def uown(part):
        return ub.at[0, pl.ds(part * hr, hr), :]

    def u_store(part):
        return pltpu.make_async_copy(uown(part), urows(0, t, part), ust_sem.at[part])

    def u_pair(part):
        return remote(uown(part), urows(1, t, part), uy_s.at[part], uy_r.at[part], pair)

    def u_copy(yy, d, part):
        ref = urows(yy, t, part)
        return remote(uown(part) if yy == 0 else ref, ref, ux_s.at[yy, d, part], ux_r.at[yy, d, part], xnb[d])

    def u_fwd(yy, d):
        ref = urows(yy, (tl, tr)[d], d)
        return remote(ref, ref, uf_s.at[yy, d], uf_r.at[yy, d], xnb[d])

    SIB = ((t, 0), (t, 1), (tl, 0), (tr, 0), (tl, 1), (tr, 1), (tf, 0), (tf, 1))

    def u_sib(yy, i):
        ref = urows(yy, *SIB[i])
        return remote(uown(i) if yy == 0 and i < 2 else ref, ref, ub_s.at[yy, i], ub_r.at[yy, i], sib)

    def u_start(yy, part):
        for d in range(2):
            u_copy(yy, d, part).start()

    def u_near(yy, part):
        for d in range(2):
            u_copy(yy, d, part).wait_recv()
            u_sib(yy, 2 + 2 * part + d).start()

    def u_far(yy):
        for d in range(2):
            u_fwd(yy, d).wait_recv()
            u_sib(yy, 6 + d).start()

    for part in range(2):
        normalize(part)
        u_start(0, part)
        u_pair(part).start()
    for i in range(2):
        u_sib(0, i).start()
        u_store(i).start()
    for m in range(1, K1):
        s_copy((m % 2) * 3 + m // 2).start()
    for k in range(K1):
        own_w(k).start()

    def block(q):
        e, g = lax.div(q, 12), lax.div(q, 14)
        i = q + 2 * lax.div(q, 6) * (1 - e) - 6 * (e - g)
        yy = lax.div(i, n_tp)
        m = lax.div(lax.rem(i, n_tp), 2)
        off = lax.div(m * (m + 1), 2)
        return yy, lax.rem(x + off, n_x) * 2 + lax.rem(i, 2)

    def up(n, blk, m0, m1, event=None):
        def loads(idx):
            yy, tt = block(blk(idx))
            s = lax.rem(idx, 2)
            return [
                pltpu.make_async_copy(
                    u_ref.at[yy, tt, pl.ds(p * lr, lr), :], ub.at[s, pl.ds(p * lr, lr), :], ld_sem.at[s, p]
                )
                for p in range(R // lr)
            ]

        for cp in loads(0):
            cp.start()

        @pl.loop(0, n)
        def _(idx):
            if event is not None:
                event(idx)

            @pl.when(idx + 1 < n)
            def _():
                for cp in loads(idx + 1):
                    cp.start()

            for cp in loads(idx):
                cp.wait()
            yy, tt = block(blk(idx))
            rows = pl.ds(pl.multiple_of((yy * n_tp + tt) * R, 16), R)

            @pl.loop(m0(idx), m1(idx))
            def _(m):
                k = kseq(m)
                pre = jnp.dot(ub[lax.rem(idx, 2)], wb[k], preferred_element_type=F32)
                h[rows, cols(k, cf)] = jax.nn.gelu(pre, approximate=True).astype(BF16)

    def s_event(m):
        s_copy(sseq(m)).wait_recv()
        f_copy(sseq(m)).start()

    def w_ready(m):
        k = kseq(m)
        d_copy(k).wait_recv()
        f_recv(k).wait_recv()

    def same(v):
        return lambda idx: v

    def straight(idx):
        return idx

    s_event(0)
    u_near(0, 0)
    u_pair(0).wait_recv()
    u_start(1, 0)
    u_sib(1, 0).start()
    u_near(0, 1)
    u_pair(1).wait_recv()
    u_start(1, 1)
    for d in range(2):
        u_fwd(0, d).start()
    u_sib(1, 1).start()
    s_event(1)
    u_near(1, 0)
    s_event(2)
    for i in range(6):
        u_sib(0, i).wait_recv()
    for i in range(2):
        u_sib(1, i).wait_recv()
    for k in range(K1):
        own_w(k).wait()
    for i in range(2):
        u_store(i).wait()
        u_pair(i).wait_send()
        u_sib(0, i).wait_send()
        for d in range(2):
            u_copy(0, d, i).wait_send()

    s_event(3)
    w_ready(0)
    w_ready(1)

    def event1(idx):
        @pl.when(idx == 3)
        def _():
            u_near(1, 1)
            for d in range(2):
                u_fwd(1, d).start()

    up(8, straight, same(0), same(2), event1)
    s_event(4)
    w_ready(2)
    for i in range(2, 6):
        u_sib(1, i).wait_recv()
    up(4, lambda idx: idx + 8, same(0), same(3))
    s_event(5)
    for j in range(SLOTS):
        wo_copy(j).start()
    w_ready(3)

    def event2(idx):
        @pl.when(idx == 3)
        def _():
            u_far(0)

    up(8, straight, same(2), same(4), event2)
    w_ready(4)

    def first6(idx):
        return lax.div(21 - idx, 16)

    def last_m0(idx):
        e = first6(idx)
        return e * (3 - 3 * lax.div(idx + 18, 22)) + (1 - e) * (4 + lax.div(idx, 14) - 5 * lax.div(idx, 20))

    def last_event(idx):
        @pl.when(idx == 3)
        def _():
            for i in range(6, 8):
                u_sib(0, i).wait_recv()

        @pl.when(idx == 6)
        def _():
            w_ready(5)

        @pl.when(idx == 10)
        def _():
            u_far(1)

        @pl.when(idx == 14)
        def _():
            fetch(0)

        @pl.when(idx == 19)
        def _():
            for i in range(6, 8):
                u_sib(1, i).wait_recv()

    up(22, lambda idx: idx - 6 + 14 * first6(idx), last_m0, lambda idx: K1 - first6(idx), last_event)

    for k in range(K1):
        f_copy(k).wait_send()
        d_copy(k).wait_send()
        s_copy(k).wait_send()

    def sib_copy(j):
        w = narrow(j)
        return remote(sibst.at[:, :, :, w], sibr.at[s2(j), :, :, :, w], sb_s, sb_r.at[s2(j)], sib)

    def yey_copy(j):
        w = narrow(j)
        src = own.at[s4(j), 1, :, pl.ds(RX, R - RX), w]
        return remote(src, yey.at[s4(j), :, :, w], yey_s.at[s2(j)], yey_r.at[s4(j)], pair)

    def yex_copy(j):
        w = narrow(j)
        return remote(own.at[s4(j), 1, x, pl.ds(0, RX), w], yex.at[s4(j), :, w], yex_s.at[s2(j)], yex_r.at[s4(j)], pair)

    def fx_copy(j, d):
        w = narrow(j)
        src = own.at[s4(j), :, xf, pl.ds(d * hx, hx), w]
        return remote(src, fx.at[s4(j), d, :, :, w], fx_s.at[s2(j), d], fx_r.at[s4(j), d], xnb[d])

    def nx_copy(j, d):
        w = narrow(j)
        src = own.at[s4(j), :, (xr, xl)[d], pl.ds(0, RX), w]
        return remote(src, nx.at[s4(j), d, :, :, w], nx_s.at[s2(j), d], nx_r.at[s4(j), d], xnb[d])

    def fy_copy(j, d):
        w = narrow(j)
        src = own.at[s4(j), 0, xf, pl.ds(RX + d * hy, hy), w]
        return remote(src, fy.at[s4(j), d, :, w], fy_s.at[s2(j), d], fy_r.at[s4(j), d], xnb[d])

    def ny_copy(j, d):
        w = narrow(j)
        src = own.at[s4(j), 0, (xr, xl)[d], pl.ds(RX, R - RX), w]
        return remote(src, ny.at[s4(j), d, :, w], ny_s.at[s2(j), d], ny_r.at[s4(j), d], xnb[d])

    def out_copy(j):
        return pltpu.make_async_copy(hid_v.at[:, dcols(j)], out_ref.at[:, dcols(j)], out_sem.at[j])

    def when_static(cond, fn):
        if isinstance(cond, bool):
            if cond:
                fn()
        else:
            pl.when(cond)(fn)

    def send(copy, j, *a):
        when_static(j >= 2, lambda: copy(j - 2, *a).wait_send())
        copy(j, *a).start()

    def down(j):
        W = slice(0, width(j))
        for cp in w2_loads(j):
            cp.wait()

        if isinstance(j, int):
            if j < N:
                fetch(j + 1)
        else:
            pl.when(j + 1 < N - 1)(lambda: fetch(j + 1))
            pl.when(j + 1 == N - 1)(lambda: fetch(N - 1))
        when_static(j >= 1, lambda: sib_copy(j - 1).wait_send())

        def part(i, cc):
            yy, xx = lax.div(i, n_x), lax.rem(i, n_x)
            rows = pl.ds(pl.multiple_of((yy * n_tp + xx * 2 + cc) * R, 16), R)
            return jnp.dot(h[rows, :], w2b[s2(j), :, W], preferred_element_type=F32)

        @pl.loop(0, 2 * n_x)
        def _(i):
            sibst[lax.div(i, n_x), lax.rem(i, n_x), :, W] = part(i, 1 - c)

        sib_copy(j).start()

        @pl.loop(0, 2 * n_x)
        def _(i):
            own[s4(j), lax.div(i, n_x), lax.rem(i, n_x), :, W] = part(i, c)

    def stage1(j):
        W = slice(0, width(j))
        sib_copy(j).wait_recv()

        @pl.loop(0, 2 * n_x)
        def _(i):
            yy, xx = lax.div(i, n_x), lax.rem(i, n_x)
            own[s4(j), yy, xx, :, W] = own[s4(j), yy, xx, :, W] + sibr[s2(j), yy, xx, :, W]

        send(yey_copy, j)
        for d in range(2):
            send(fx_copy, j, d)

    def stage2(j):
        s, W = s4(j), slice(0, width(j))
        for d in range(2):
            fx_copy(j, d).wait_recv()
            b, rows = (xr, xl)[d], slice(d * hx, (d + 1) * hx)
            for yy in range(2):
                own[s, yy, b, rows, W] = own[s, yy, b, rows, W] + fx[s, d, yy, :, W]
        for d in range(2):
            send(nx_copy, j, d)
        yey_copy(j).wait_recv()

        @pl.loop(0, n_x)
        def _(i):
            own[s, 0, i, RX:, W] = own[s, 0, i, RX:, W] + yey[s, i, :, W]

        for d in range(2):
            send(fy_copy, j, d)

    def stage3(j):
        s, W = s4(j), slice(0, width(j))
        for d in range(2):
            fy_copy(j, d).wait_recv()
            b, rows = (xr, xl)[d], slice(RX + d * hy, RX + (d + 1) * hy)
            own[s, 0, b, rows, W] = own[s, 0, b, rows, W] + fy[s, d, :, W]
        for d in range(2):
            ny_copy(j, d).start()
        for d in range(2):
            nx_copy(j, d).wait_recv()
        for yy in (1, 0):
            own[s, yy, x, :RX, W] = own[s, yy, x, :RX, W] + nx[s, 0, yy, :, W] + nx[s, 1, yy, :, W]
        yex_copy(j).start()

    def stage4(j):
        s, W = s4(j), slice(0, width(j))
        for d in range(2):
            ny_copy(j, d).wait_recv()
        lo = own[s, 0, x, RX:, W] + ny[s, 0, :, W] + ny[s, 1, :, W]
        hid_v[RX:, dcols(j)] = (hid_v[RX:, dcols(j)].astype(F32) + lo).astype(BF16)
        yex_copy(j).wait_recv()
        hi = own[s, 0, x, :RX, W] + yex[s, :, W]
        hid_v[:RX, dcols(j)] = (hid_v[:RX, dcols(j)].astype(F32) + hi).astype(BF16)
        out_copy(j).start()
        yex_copy(j).wait_send()
        for d in range(2):
            ny_copy(j, d).wait_send()

    @pl.loop(0, N - 1)
    def _(j):
        @pl.when(j + SLOTS < N)
        def _():
            wo_copy(j + SLOTS).start()

        down(j)
        stage1(j)
        pl.when(j >= 1)(lambda: stage2(j - 1))
        pl.when(j >= 2)(lambda: stage3(j - 2))
        pl.when(j >= 3)(lambda: stage4(j - 3))

    for j in range(N - 1, N + 4):
        if j <= N:
            down(j)
            stage1(j)
        for lag, stage in ((1, stage2), (2, stage3), (3, stage4)):
            if j - lag <= N:
                stage(j - lag)

    for yy in range(2):
        for d in range(2):
            u_fwd(yy, d).wait_send()
            if yy == 1:
                for part in range(2):
                    u_copy(yy, d, part).wait_send()
        for i in range(2 * (1 - yy), 8):
            u_sib(yy, i).wait_send()
    sib_copy(N).wait_send()
    for j in (N - 1, N):
        yey_copy(j).wait_send()
        for d in range(2):
            for copy in (fx_copy, nx_copy, fy_copy):
                copy(j, d).wait_send()

    @pl.loop(0, N)
    def _(j):
        wo_copy(j).wait_send()

    @pl.loop(0, N - 1)
    def _(j):
        out_copy(j).wait()

    for j in (N - 1, N):
        out_copy(j).wait()


def make_local(n_tp, n_y, N):
    def local_mlp(hidden, ln_scale, w_in, w_out):
        R, D = hidden.shape
        sub = w_out.shape[0]
        cd = D // N
        n_x = n_tp // 2
        RX = split_rows(R)
        any_spec = pl.BlockSpec(memory_space=pl.ANY)
        dma = pltpu.SemaphoreType.DMA
        vm = pltpu.VMEM
        S = SLOTS
        out, _, _ = pl.pallas_call(
            functools.partial(mlp_kernel, n_tp, n_y, N),
            out_shape=(
                jax.ShapeDtypeStruct((R, D), BF16),
                jax.ShapeDtypeStruct((2, n_tp, R, D), BF16),
                jax.ShapeDtypeStruct((sub, D), BF16),
            ),
            in_specs=[any_spec, pl.BlockSpec(memory_space=vm), any_spec, any_spec],
            out_specs=(any_spec, any_spec, any_spec),
            scratch_shapes=[
                vm((6, D, sub // 3), BF16),
                vm((2 * n_tp * R, 2 * sub), BF16),
                vm((2, 2 * sub, cd), BF16),
                vm((2, R, D), BF16),
                vm((R, D), BF16),
                vm((S, 2, n_x, R, cd), F32),
                vm((2, n_x, R, cd), F32),
                vm((2, 2, n_x, R, cd), F32),
                vm((S, n_x, R - RX, cd), F32),
                vm((S, 2, 2, RX // 2, cd), F32),
                vm((S, 2, 2, RX, cd), F32),
                vm((S, 2, (R - RX) // 2, cd), F32),
                vm((S, 2, R - RX, cd), F32),
                vm((S, RX, cd), F32),
                dma((2,)), dma((2,)), dma((2, 4)), dma((6,)), dma((2, 2)), dma((N + 1,)),
                dma((6,)), dma((6,)), dma((6,)), dma((6,)), dma((6,)), dma((6,)), dma((N,)), dma((N,)),
                dma((2,)), dma((2,)), dma((2, 2, 2)), dma((2, 2, 2)), dma((2, 2)), dma((2, 2)), dma((2, 8)), dma((2, 8)),
                dma, dma((2,)), dma((2,)), dma((S,)), dma((2, 2)), dma((S, 2)), dma((2, 2)), dma((S, 2)),
                dma((2, 2)), dma((S, 2)), dma((2, 2)), dma((S, 2)), dma((2,)), dma((S,)),
            ],
            compiler_params=pltpu.CompilerParams(
                collective_id=0, has_side_effects=True, vmem_limit_bytes=67043328
            ),
            cost_estimate=pl.CostEstimate(
                flops=4 * n_tp * R * D * w_in.shape[1], bytes_accessed=8 * D * w_in.shape[1], transcendentals=0
            ),
            name="mlp",
        )(hidden, ln_scale.reshape(1, D), w_in, w_out)
        return out

    return local_mlp


def solution(mesh):
    return jax.shard_map(
        make_local(mesh.shape["tp"], mesh.shape["fsdp"], CHUNKS),
        mesh=mesh,
        in_specs=(P(("data", "fsdp", "tp"), None), P(None), P("fsdp", "tp"), P(("tp", "fsdp"), None)),
        out_specs=P(("data", "fsdp", "tp"), None),
        check_vma=False,
    )
```

```python
import functools

import jax
import jax.numpy as jnp
from jax import lax
from jax.experimental import pallas as pl
from jax.experimental.pallas import tpu as pltpu
from jax.sharding import PartitionSpec as P

LN_EPS = 1e-6
CHUNKS = 24
F32 = jnp.float32
BF16 = jnp.bfloat16
SLOTS = 4
NB = 5


def split_rows(R):
    return R * 9 // 16 // 16 * 16


def mlp_kernel(
    n_tp, n_y, N, hid_ref, scale_ref, win_ref, wout_ref, out_ref, u_ref, gout_ref,
    wb, h, w2b, hid_v, sibr, yey, fx, nx, fy, ny, yex,
    hid_sem, ust_sem, ld_sem, ow_sem, w2_sem, out_sem,
    d_s, d_r, s_s, s_r, f_s, f_r, wo_s, wo_r,
    uy_s, uy_r, ux_s, ux_r, uf_s, uf_r, ub_s, ub_r,
    sb_s, sb_r, yey_s, yey_r, fx_s, fx_r, nx_s, nx_r, fy_s, fy_r, ny_s, ny_r, yex_s, yex_r,
):
    R, D = hid_v.shape
    sub = wout_ref.shape[0]
    dk = win_ref.shape[0]
    K1 = 6
    cf, cd = sub // 3, D // N
    n_x = n_tp // 2
    RX = split_rows(R)
    hx, hy = RX // 2, (R - RX) // 2
    t = lax.axis_index("tp")
    y = lax.axis_index("fsdp")
    x, c = lax.div(t, 2), lax.rem(t, 2)
    xr, xl, xf = lax.rem(x + 1, n_x), lax.rem(x + n_x - 1, n_x), lax.rem(x + 2, n_x)
    tr, tl, tf = xr * 2 + c, xl * 2 + c, xf * 2 + c
    tsib = x * 2 + 1 - c
    yp = lax.div(y, 2) * 2 + 1 - lax.rem(y, 2)
    yd = n_y - 1 - y
    yo = n_y - 1 - yp
    pair, other, sib = {"fsdp": yp}, {"fsdp": yd}, {"tp": tsib}
    xnb = ({"tp": tr}, {"tp": tl})

    def remote(src, dst, s, r, dev):
        return pltpu.make_async_remote_copy(
            src_ref=src, dst_ref=dst, send_sem=s, recv_sem=r, device_id=dev, device_id_type=pl.DeviceIdType.MESH
        )

    def cols(k, n):
        return pl.ds(pl.multiple_of(k * n, 128), n)

    def wrows(o):
        return pl.ds(pl.multiple_of(o * dk, 16), dk)

    def sseq(m):
        return lax.rem(m, 2) * 3 + lax.div(m, 2)

    def kseq(m):
        return lax.rem(m + 1, 2) * 3 + lax.div(m, 2)

    def win_cols(first, second, k):
        s = jnp.where(k < 3, first, second) if not isinstance(k, int) else (first if k < 3 else second)
        return pl.ds(pl.multiple_of(s * sub + lax.rem(k, 3) * cf, 128), cf)

    def own_w(k):
        return pltpu.make_async_copy(
            win_ref.at[:, win_cols(y, yd, k)], wb.at[k, wrows(y)], ow_sem.at[k]
        )

    def d_copy(k):
        return remote(
            win_ref.at[:, win_cols(yd, y, k)], wb.at[k, wrows(y)], d_s.at[k], d_r.at[k], other
        )

    def s_copy(k):
        return remote(
            win_ref.at[:, win_cols(yp, yo, k)], wb.at[k, wrows(y)], s_s.at[k], s_r.at[k], pair
        )

    def f_copy(k):
        kk = lax.rem(k + 3, K1)
        return remote(
            wb.at[k, wrows(yp)], wb.at[kk, wrows(yp)], f_s.at[kk], f_r.at[kk], other
        )

    def f_recv(k):
        return remote(wb.at[k, wrows(yo)], wb.at[k, wrows(yo)], f_s.at[k], f_r.at[k], other)

    def wo_copy(j):
        return remote(wout_ref.at[:, cols(j, cd)], gout_ref.at[:, cols(j, cd)], wo_s.at[j], wo_r.at[j], other)

    def s2(j):
        return lax.rem(j, 2)

    def s4(j):
        return lax.rem(j, SLOTS)

    def width(j):
        return cd // 2 if isinstance(j, int) and j >= N - 1 else cd

    def dcols(j):
        if width(j) == cd:
            return cols(j, cd)
        return pl.ds((N - 1) * cd + (j - N + 1) * (cd // 2), cd // 2)

    def narrow(j):
        return pl.ds(0, width(j))

    def w2_loads(j):
        lo, hi, w = pl.ds(0, sub), pl.ds(sub, sub), narrow(j)
        return (
            pltpu.make_async_copy(wout_ref.at[:, dcols(j)], w2b.at[s2(j), lo, w], w2_sem.at[s2(j), 0]),
            pltpu.make_async_copy(gout_ref.at[:, dcols(j)], w2b.at[s2(j), hi, w], w2_sem.at[s2(j), 1]),
        )

    def fetch(j):
        if not (isinstance(j, int) and j == N):
            wo_copy(j).wait_recv()
        for cp in w2_loads(j):
            cp.start()

    barrier = pltpu.get_barrier_semaphore()
    for dev in (pair, other, *xnb, sib):
        pl.semaphore_signal(barrier, inc=1, device_id=dev, device_id_type=pl.DeviceIdType.MESH)

    def hid_load(part):
        rows = pl.ds(part * (R // 2), R // 2)
        return pltpu.make_async_copy(hid_ref.at[rows], hid_v.at[rows], hid_sem.at[part])

    for part in range(2):
        hid_load(part).start()
    pl.semaphore_wait(barrier, 5)

    for m in range(2):
        s_copy((m % 2) * 3 + m // 2).start()
        d_copy(((m + 1) % 2) * 3 + m // 2).start()

    def phase1(ub):
        TR = 16
        hr = R // 2
        lr = max(R // 4, 16)

        def normalize(part):
            hid_load(part).wait()

            @pl.loop(0, hr // TR)
            def _(i):
                rows = pl.ds(pl.multiple_of(part * hr + i * TR, TR), TR)
                v = hid_v[rows, :].astype(F32)
                cen = v - jnp.mean(v, axis=-1, keepdims=True)
                var = jnp.mean(cen * cen, axis=-1, keepdims=True)
                ub[0, rows, :] = (cen * lax.rsqrt(var + LN_EPS) * scale_ref[...]).astype(BF16)

        def urows(yy, tt, part):
            return u_ref.at[yy, tt, pl.ds(part * hr, hr), :]

        def uown(part):
            return ub.at[0, pl.ds(part * hr, hr), :]

        def u_store(part):
            return pltpu.make_async_copy(uown(part), urows(0, t, part), ust_sem.at[part])

        def u_pair(part):
            return remote(uown(part), urows(1, t, part), uy_s.at[part], uy_r.at[part], pair)

        def u_copy(yy, d, part):
            ref = urows(yy, t, part)
            return remote(uown(part) if yy == 0 else ref, ref, ux_s.at[yy, d, part], ux_r.at[yy, d, part], xnb[d])

        def u_fwd(yy, d):
            ref = urows(yy, (tl, tr)[d], d)
            return remote(ref, ref, uf_s.at[yy, d], uf_r.at[yy, d], xnb[d])

        SIB = ((t, 0), (t, 1), (tl, 0), (tr, 0), (tl, 1), (tr, 1), (tf, 0), (tf, 1))

        def u_sib(yy, i):
            ref = urows(yy, *SIB[i])
            return remote(uown(i) if yy == 0 and i < 2 else ref, ref, ub_s.at[yy, i], ub_r.at[yy, i], sib)

        def u_start(yy, part):
            for d in range(2):
                u_copy(yy, d, part).start()

        def u_near(yy, part):
            for d in range(2):
                u_copy(yy, d, part).wait_recv()
                u_sib(yy, 2 + 2 * part + d).start()

        def u_far(yy):
            for d in range(2):
                u_fwd(yy, d).wait_recv()
                u_sib(yy, 6 + d).start()

        for part in range(2):
            normalize(part)
            u_start(0, part)
            u_pair(part).start()
        for i in range(2):
            u_sib(0, i).start()
            u_store(i).start()
        for m in range(2, K1):
            s_copy((m % 2) * 3 + m // 2).start()
        for k in range(K1):
            own_w(k).start()

        def block(q):
            e, g = lax.div(q, 12), lax.div(q, 14)
            i = q + 2 * lax.div(q, 6) * (1 - e) - 6 * (e - g)
            yy = lax.div(i, n_tp)
            m = lax.div(lax.rem(i, n_tp), 2)
            off = lax.div(m * (m + 1), 2)
            return yy, lax.rem(x + off, n_x) * 2 + lax.rem(i, 2)

        def up(n, blk, m0, m1, event=None):
            def loads(idx):
                yy, tt = block(blk(idx))
                s = lax.rem(idx, NB)
                return [
                    pltpu.make_async_copy(
                        u_ref.at[yy, tt, pl.ds(p * lr, lr), :], ub.at[s, pl.ds(p * lr, lr), :], ld_sem.at[s, p]
                    )
                    for p in range(R // lr)
                ]

            for i in range(min(NB - 1, n)):
                for cp in loads(i):
                    cp.start()

            @pl.loop(0, n)
            def _(idx):
                if event is not None:
                    event(idx)

                @pl.when(idx + NB - 1 < n)
                def _():
                    for cp in loads(idx + NB - 1):
                        cp.start()

                for cp in loads(idx):
                    cp.wait()
                yy, tt = block(blk(idx))
                rows = pl.ds(pl.multiple_of((yy * n_tp + tt) * R, 16), R)

                @pl.loop(m0(idx), m1(idx))
                def _(m):
                    k = kseq(m)
                    pre = jnp.dot(ub[lax.rem(idx, NB)], wb[k], preferred_element_type=F32)
                    h[rows, cols(k, cf)] = jax.nn.gelu(pre, approximate=True).astype(BF16)

        def s_event(m):
            s_copy(sseq(m)).wait_recv()
            f_copy(sseq(m)).start()

        def w_ready(m):
            k = kseq(m)
            d_copy(k).wait_recv()
            f_recv(k).wait_recv()

        def same(v):
            return lambda idx: v

        def straight(idx):
            return idx

        s_event(0)
        s_event(1)
        for m in range(2, K1):
            d_copy(((m + 1) % 2) * 3 + m // 2).start()
        u_near(0, 0)
        u_pair(0).wait_recv()
        u_start(1, 0)
        u_sib(1, 0).start()
        u_near(0, 1)
        u_pair(1).wait_recv()
        u_start(1, 1)
        for d in range(2):
            u_fwd(0, d).start()
        u_sib(1, 1).start()
        u_near(1, 0)
        for i in range(6):
            u_sib(0, i).wait_recv()
        for i in range(2):
            u_sib(1, i).wait_recv()
        for k in range(K1):
            own_w(k).wait()
        for i in range(2):
            u_store(i).wait()
            u_pair(i).wait_send()
            u_sib(0, i).wait_send()
            for d in range(2):
                u_copy(0, d, i).wait_send()

        w_ready(0)
        w_ready(1)

        def event1(idx):
            @pl.when(idx == 5)
            def _():
                s_event(2)

        up(8, straight, same(0), same(2), event1)
        s_event(3)
        u_near(1, 1)
        for d in range(2):
            u_fwd(1, d).start()
        for i in range(2, 6):
            u_sib(1, i).wait_recv()
        up(4, lambda idx: idx + 8, same(0), same(2))
        s_event(4)
        w_ready(2)
        up(12, straight, same(2), same(3))
        s_event(5)
        for j in range(SLOTS):
            wo_copy(j).start()
        w_ready(3)

        def event2(idx):
            @pl.when(idx == 5)
            def _():
                u_far(0)

        up(12, straight, same(3), same(4), event2)
        w_ready(4)
        for i in range(6, 8):
            u_sib(0, i).wait_recv()

        def first2(idx):
            return lax.div(25 - idx, 24)

        def last_block(idx):
            g = lax.div(idx, 20)
            return idx - 2 + 14 * first2(idx) - 12 * (lax.div(idx, 14) - g) - 6 * g

        def last_event(idx):
            @pl.when(idx == 8)
            def _():
                w_ready(5)

            @pl.when(idx == 12)
            def _():
                u_far(1)

            @pl.when(idx == 15)
            def _():
                fetch(0)

            @pl.when(idx == 18)
            def _():
                for i in range(6, 8):
                    u_sib(1, i).wait_recv()

        up(
            24,
            last_block,
            lambda idx: (1 - first2(idx)) * (4 + lax.div(idx, 14)) - 5 * lax.div(idx, 22),
            lambda idx: 5 + lax.div(idx + 16, 24),
            last_event,
        )

        for yy in range(2):
            for d in range(2):
                u_fwd(yy, d).wait_send()
                if yy == 1:
                    for part in range(2):
                        u_copy(yy, d, part).wait_send()
            for i in range(2 * (1 - yy), 8):
                u_sib(yy, i).wait_send()

    pl.run_scoped(phase1, pltpu.VMEM((NB, R, D), BF16))

    for k in range(K1):
        f_copy(k).wait_send()
        d_copy(k).wait_send()
        s_copy(k).wait_send()

    def phase2(own, sibst):
        def sib_copy(j):
            w = narrow(j)
            return remote(sibst.at[:, :, :, w], sibr.at[s2(j), :, :, :, w], sb_s, sb_r.at[s2(j)], sib)

        def yey_copy(j):
            w = narrow(j)
            src = own.at[s4(j), 1, :, pl.ds(RX, R - RX), w]
            return remote(src, yey.at[s4(j), :, :, w], yey_s.at[s2(j)], yey_r.at[s4(j)], pair)

        def yex_copy(j):
            w = narrow(j)
            return remote(own.at[s4(j), 1, x, pl.ds(0, RX), w], yex.at[s4(j), :, w], yex_s.at[s2(j)], yex_r.at[s4(j)], pair)

        def fx_copy(j, d):
            w = narrow(j)
            src = own.at[s4(j), :, xf, pl.ds(d * hx, hx), w]
            return remote(src, fx.at[s4(j), d, :, :, w], fx_s.at[s2(j), d], fx_r.at[s4(j), d], xnb[d])

        def nx_copy(j, d):
            w = narrow(j)
            src = own.at[s4(j), :, (xr, xl)[d], pl.ds(0, RX), w]
            return remote(src, nx.at[s4(j), d, :, :, w], nx_s.at[s2(j), d], nx_r.at[s4(j), d], xnb[d])

        def fy_copy(j, d):
            w = narrow(j)
            src = own.at[s4(j), 0, xf, pl.ds(RX + d * hy, hy), w]
            return remote(src, fy.at[s4(j), d, :, w], fy_s.at[s2(j), d], fy_r.at[s4(j), d], xnb[d])

        def ny_copy(j, d):
            w = narrow(j)
            src = own.at[s4(j), 0, (xr, xl)[d], pl.ds(RX, R - RX), w]
            return remote(src, ny.at[s4(j), d, :, w], ny_s.at[s2(j), d], ny_r.at[s4(j), d], xnb[d])

        def out_copy(j):
            return pltpu.make_async_copy(hid_v.at[:, dcols(j)], out_ref.at[:, dcols(j)], out_sem.at[j])

        def when_static(cond, fn):
            if isinstance(cond, bool):
                if cond:
                    fn()
            else:
                pl.when(cond)(fn)

        def send(copy, j, *a):
            when_static(j >= 2, lambda: copy(j - 2, *a).wait_send())
            copy(j, *a).start()

        def down(j):
            W = slice(0, width(j))
            for cp in w2_loads(j):
                cp.wait()

            if isinstance(j, int):
                if j < N:
                    fetch(j + 1)
            else:
                pl.when(j + 1 < N - 1)(lambda: fetch(j + 1))
                pl.when(j + 1 == N - 1)(lambda: fetch(N - 1))
            when_static(j >= 1, lambda: sib_copy(j - 1).wait_send())

            def part(i, cc):
                yy, xx = lax.div(i, n_x), lax.rem(i, n_x)
                rows = pl.ds(pl.multiple_of((yy * n_tp + xx * 2 + cc) * R, 16), R)
                return jnp.dot(h[rows, :], w2b[s2(j), :, W], preferred_element_type=F32)

            @pl.loop(0, 2 * n_x)
            def _(i):
                sibst[lax.div(i, n_x), lax.rem(i, n_x), :, W] = part(i, 1 - c)

            sib_copy(j).start()

            @pl.loop(0, 2 * n_x)
            def _(i):
                own[s4(j), lax.div(i, n_x), lax.rem(i, n_x), :, W] = part(i, c)

        def stage1(j):
            W = slice(0, width(j))
            sib_copy(j).wait_recv()

            @pl.loop(0, 2 * n_x)
            def _(i):
                yy, xx = lax.div(i, n_x), lax.rem(i, n_x)
                own[s4(j), yy, xx, :, W] = own[s4(j), yy, xx, :, W] + sibr[s2(j), yy, xx, :, W]

            send(yey_copy, j)
            for d in range(2):
                send(fx_copy, j, d)

        def stage2(j):
            s, W = s4(j), slice(0, width(j))
            for d in range(2):
                fx_copy(j, d).wait_recv()
                b, rows = (xr, xl)[d], slice(d * hx, (d + 1) * hx)
                for yy in range(2):
                    own[s, yy, b, rows, W] = own[s, yy, b, rows, W] + fx[s, d, yy, :, W]
            for d in range(2):
                send(nx_copy, j, d)
            yey_copy(j).wait_recv()

            @pl.loop(0, n_x)
            def _(i):
                own[s, 0, i, RX:, W] = own[s, 0, i, RX:, W] + yey[s, i, :, W]

            for d in range(2):
                send(fy_copy, j, d)

        def stage3(j):
            s, W = s4(j), slice(0, width(j))
            for d in range(2):
                fy_copy(j, d).wait_recv()
                b, rows = (xr, xl)[d], slice(RX + d * hy, RX + (d + 1) * hy)
                own[s, 0, b, rows, W] = own[s, 0, b, rows, W] + fy[s, d, :, W]
            for d in range(2):
                ny_copy(j, d).start()
            for d in range(2):
                nx_copy(j, d).wait_recv()
            for yy in (1, 0):
                own[s, yy, x, :RX, W] = own[s, yy, x, :RX, W] + nx[s, 0, yy, :, W] + nx[s, 1, yy, :, W]
            yex_copy(j).start()

        def stage4(j):
            s, W = s4(j), slice(0, width(j))
            for d in range(2):
                ny_copy(j, d).wait_recv()
            lo = own[s, 0, x, RX:, W] + ny[s, 0, :, W] + ny[s, 1, :, W]
            hid_v[RX:, dcols(j)] = (hid_v[RX:, dcols(j)].astype(F32) + lo).astype(BF16)
            yex_copy(j).wait_recv()
            hi = own[s, 0, x, :RX, W] + yex[s, :, W]
            hid_v[:RX, dcols(j)] = (hid_v[:RX, dcols(j)].astype(F32) + hi).astype(BF16)
            out_copy(j).start()
            yex_copy(j).wait_send()
            for d in range(2):
                ny_copy(j, d).wait_send()

        @pl.loop(0, N - 1)
        def _(j):
            @pl.when(j + SLOTS < N)
            def _():
                wo_copy(j + SLOTS).start()

            down(j)
            stage1(j)
            pl.when(j >= 1)(lambda: stage2(j - 1))
            pl.when(j >= 2)(lambda: stage3(j - 2))
            pl.when(j >= 3)(lambda: stage4(j - 3))

        for j in range(N - 1, N + 4):
            if j <= N:
                down(j)
                stage1(j)
            for lag, stage in ((1, stage2), (2, stage3), (3, stage4)):
                if j - lag <= N:
                    stage(j - lag)

        sib_copy(N).wait_send()
        for j in (N - 1, N):
            yey_copy(j).wait_send()
            for d in range(2):
                for copy in (fx_copy, nx_copy, fy_copy):
                    copy(j, d).wait_send()

        @pl.loop(0, N)
        def _(j):
            wo_copy(j).wait_send()

        @pl.loop(0, N - 1)
        def _(j):
            out_copy(j).wait()

        for j in (N - 1, N):
            out_copy(j).wait()

    pl.run_scoped(phase2, pltpu.VMEM((SLOTS, 2, n_x, R, cd), F32), pltpu.VMEM((2, n_x, R, cd), F32))


def make_local(n_tp, n_y, N):
    def local_mlp(hidden, ln_scale, w_in, w_out):
        R, D = hidden.shape
        sub = w_out.shape[0]
        cd = D // N
        n_x = n_tp // 2
        RX = split_rows(R)
        any_spec = pl.BlockSpec(memory_space=pl.ANY)
        dma = pltpu.SemaphoreType.DMA
        vm = pltpu.VMEM
        S = SLOTS
        out, _, _ = pl.pallas_call(
            functools.partial(mlp_kernel, n_tp, n_y, N),
            out_shape=(
                jax.ShapeDtypeStruct((R, D), BF16),
                jax.ShapeDtypeStruct((2, n_tp, R, D), BF16),
                jax.ShapeDtypeStruct((sub, D), BF16),
            ),
            in_specs=[any_spec, pl.BlockSpec(memory_space=vm), any_spec, any_spec],
            out_specs=(any_spec, any_spec, any_spec),
            scratch_shapes=[
                vm((6, D, sub // 3), BF16),
                vm((2 * n_tp * R, 2 * sub), BF16),
                vm((2, 2 * sub, cd), BF16),
                vm((R, D), BF16),
                vm((2, 2, n_x, R, cd), F32),
                vm((S, n_x, R - RX, cd), F32),
                vm((S, 2, 2, RX // 2, cd), F32),
                vm((S, 2, 2, RX, cd), F32),
                vm((S, 2, (R - RX) // 2, cd), F32),
                vm((S, 2, R - RX, cd), F32),
                vm((S, RX, cd), F32),
                dma((2,)), dma((2,)), dma((NB, 4)), dma((6,)), dma((2, 2)), dma((N + 1,)),
                dma((6,)), dma((6,)), dma((6,)), dma((6,)), dma((6,)), dma((6,)), dma((N,)), dma((N,)),
                dma((2,)), dma((2,)), dma((2, 2, 2)), dma((2, 2, 2)), dma((2, 2)), dma((2, 2)), dma((2, 8)), dma((2, 8)),
                dma, dma((2,)), dma((2,)), dma((S,)), dma((2, 2)), dma((S, 2)), dma((2, 2)), dma((S, 2)),
                dma((2, 2)), dma((S, 2)), dma((2, 2)), dma((S, 2)), dma((2,)), dma((S,)),
            ],
            compiler_params=pltpu.CompilerParams(
                collective_id=0, has_side_effects=True, vmem_limit_bytes=67043328
            ),
            cost_estimate=pl.CostEstimate(
                flops=4 * n_tp * R * D * w_in.shape[1], bytes_accessed=8 * D * w_in.shape[1], transcendentals=0
            ),
            name="mlp",
        )(hidden, ln_scale.reshape(1, D), w_in, w_out)
        return out

    return local_mlp


def solution(mesh):
    return jax.shard_map(
        make_local(mesh.shape["tp"], mesh.shape["fsdp"], CHUNKS),
        mesh=mesh,
        in_specs=(P(("data", "fsdp", "tp"), None), P(None), P("fsdp", "tp"), P(("tp", "fsdp"), None)),
        out_specs=P(("data", "fsdp", "tp"), None),
        check_vma=False,
    )
```

```python
import functools

import jax
import jax.numpy as jnp
from jax import lax
from jax.experimental import pallas as pl
from jax.experimental.pallas import tpu as pltpu
from jax.sharding import PartitionSpec as P

LN_EPS = 1e-6
CHUNKS = 24
F32 = jnp.float32
BF16 = jnp.bfloat16
SLOTS = 4
NB = 5


def split_rows(R):
    return R * 9 // 16 // 16 * 16


def mlp_kernel(
    n_tp, n_y, N, hid_ref, scale_ref, win_ref, wout_ref, out_ref, u_ref, gout_ref,
    wb, h, w2b, hid_v, sibr, yey, fx, nx, fy, ny, yex,
    hid_sem, ust_sem, ld_sem, ow_sem, w2_sem, out_sem,
    d_s, d_r, s_s, s_r, f_s, f_r, wo_s, wo_r,
    uy_s, uy_r, ux_s, ux_r, uf_s, uf_r, ub_s, ub_r,
    sb_s, sb_r, yey_s, yey_r, fx_s, fx_r, nx_s, nx_r, fy_s, fy_r, ny_s, ny_r, yex_s, yex_r,
):
    R, D = hid_v.shape
    sub = wout_ref.shape[0]
    dk = win_ref.shape[0]
    K1 = 6
    cf, cd = sub // 3, D // N
    n_x = n_tp // 2
    RX = split_rows(R)
    hx, hy = RX // 2, (R - RX) // 2
    t = lax.axis_index("tp")
    y = lax.axis_index("fsdp")
    x, c = lax.div(t, 2), lax.rem(t, 2)
    xr, xl, xf = lax.rem(x + 1, n_x), lax.rem(x + n_x - 1, n_x), lax.rem(x + 2, n_x)
    tr, tl, tf = xr * 2 + c, xl * 2 + c, xf * 2 + c
    tsib = x * 2 + 1 - c
    yp = lax.div(y, 2) * 2 + 1 - lax.rem(y, 2)
    yd = n_y - 1 - y
    yo = n_y - 1 - yp
    pair, other, sib = {"fsdp": yp}, {"fsdp": yd}, {"tp": tsib}
    xnb = ({"tp": tr}, {"tp": tl})

    def remote(src, dst, s, r, dev):
        return pltpu.make_async_remote_copy(
            src_ref=src, dst_ref=dst, send_sem=s, recv_sem=r, device_id=dev, device_id_type=pl.DeviceIdType.MESH
        )

    def cols(k, n):
        return pl.ds(pl.multiple_of(k * n, 128), n)

    def wrows(o):
        return pl.ds(pl.multiple_of(o * dk, 16), dk)

    def sseq(m):
        return lax.rem(m, 2) * 3 + lax.div(m, 2)

    def kseq(m):
        return lax.rem(m + 1, 2) * 3 + lax.div(m, 2)

    def win_cols(first, second, k):
        s = jnp.where(k < 3, first, second) if not isinstance(k, int) else (first if k < 3 else second)
        return pl.ds(pl.multiple_of(s * sub + lax.rem(k, 3) * cf, 128), cf)

    def own_w(k):
        return pltpu.make_async_copy(
            win_ref.at[:, win_cols(y, yd, k)], wb.at[k, wrows(y)], ow_sem.at[k]
        )

    def d_copy(k):
        return remote(
            win_ref.at[:, win_cols(yd, y, k)], wb.at[k, wrows(y)], d_s.at[k], d_r.at[k], other
        )

    def s_copy(k):
        return remote(
            win_ref.at[:, win_cols(yp, yo, k)], wb.at[k, wrows(y)], s_s.at[k], s_r.at[k], pair
        )

    def f_copy(k):
        kk = lax.rem(k + 3, K1)
        return remote(
            wb.at[k, wrows(yp)], wb.at[kk, wrows(yp)], f_s.at[kk], f_r.at[kk], other
        )

    def f_recv(k):
        return remote(wb.at[k, wrows(yo)], wb.at[k, wrows(yo)], f_s.at[k], f_r.at[k], other)

    def wo_copy(j):
        return remote(wout_ref.at[:, cols(j, cd)], gout_ref.at[:, cols(j, cd)], wo_s.at[j], wo_r.at[j], other)

    def s2(j):
        return lax.rem(j, 2)

    def s4(j):
        return lax.rem(j, SLOTS)

    def width(j):
        return cd // 2 if isinstance(j, int) and j >= N - 1 else cd

    def dcols(j):
        if width(j) == cd:
            return cols(j, cd)
        return pl.ds((N - 1) * cd + (j - N + 1) * (cd // 2), cd // 2)

    def narrow(j):
        return pl.ds(0, width(j))

    def w2_loads(j):
        lo, hi, w = pl.ds(0, sub), pl.ds(sub, sub), narrow(j)
        return (
            pltpu.make_async_copy(wout_ref.at[:, dcols(j)], w2b.at[s2(j), lo, w], w2_sem.at[s2(j), 0]),
            pltpu.make_async_copy(gout_ref.at[:, dcols(j)], w2b.at[s2(j), hi, w], w2_sem.at[s2(j), 1]),
        )

    def fetch(j):
        if not (isinstance(j, int) and j == N):
            wo_copy(j).wait_recv()
        for cp in w2_loads(j):
            cp.start()

    barrier = pltpu.get_barrier_semaphore()
    for dev in (pair, other, *xnb, sib):
        pl.semaphore_signal(barrier, inc=1, device_id=dev, device_id_type=pl.DeviceIdType.MESH)

    def hid_load(part):
        rows = pl.ds(part * (R // 2), R // 2)
        return pltpu.make_async_copy(hid_ref.at[rows], hid_v.at[rows], hid_sem.at[part])

    for part in range(2):
        hid_load(part).start()
    pl.semaphore_wait(barrier, 5)

    for m in range(2):
        s_copy((m % 2) * 3 + m // 2).start()
        d_copy(((m + 1) % 2) * 3 + m // 2).start()

    def phase1(ub):
        TR = 16
        hr = R // 2
        lr = max(R // 4, 16)

        def normalize(part):
            hid_load(part).wait()

            @pl.loop(0, hr // TR)
            def _(i):
                rows = pl.ds(pl.multiple_of(part * hr + i * TR, TR), TR)
                v = hid_v[rows, :].astype(F32)
                cen = v - jnp.mean(v, axis=-1, keepdims=True)
                var = jnp.mean(cen * cen, axis=-1, keepdims=True)
                ub[0, rows, :] = (cen * lax.rsqrt(var + LN_EPS) * scale_ref[...]).astype(BF16)

        def urows(yy, tt, part):
            return u_ref.at[yy, tt, pl.ds(part * hr, hr), :]

        def uown(part):
            return ub.at[0, pl.ds(part * hr, hr), :]

        def u_store(part):
            return pltpu.make_async_copy(uown(part), urows(0, t, part), ust_sem.at[part])

        def u_pair(part):
            return remote(uown(part), urows(1, t, part), uy_s.at[part], uy_r.at[part], pair)

        def u_copy(yy, d, part):
            ref = urows(yy, t, part)
            return remote(uown(part) if yy == 0 else ref, ref, ux_s.at[yy, d, part], ux_r.at[yy, d, part], xnb[d])

        def u_fwd(yy, d):
            ref = urows(yy, (tl, tr)[d], d)
            return remote(ref, ref, uf_s.at[yy, d], uf_r.at[yy, d], xnb[d])

        SIB = ((t, 0), (t, 1), (tl, 0), (tr, 0), (tl, 1), (tr, 1), (tf, 0), (tf, 1))

        def u_sib(yy, i):
            ref = urows(yy, *SIB[i])
            return remote(uown(i) if yy == 0 and i < 2 else ref, ref, ub_s.at[yy, i], ub_r.at[yy, i], sib)

        def u_start(yy, part):
            for d in range(2):
                u_copy(yy, d, part).start()

        def u_near(yy, part):
            for d in range(2):
                u_copy(yy, d, part).wait_recv()
                u_sib(yy, 2 + 2 * part + d).start()

        def u_far(yy):
            for d in range(2):
                u_fwd(yy, d).wait_recv()
                u_sib(yy, 6 + d).start()

        for part in range(2):
            normalize(part)
            u_start(0, part)
            u_pair(part).start()
        for i in range(2):
            u_sib(0, i).start()
            u_store(i).start()
        for m in range(2, K1):
            s_copy((m % 2) * 3 + m // 2).start()
        for k in range(K1):
            own_w(k).start()

        def block(q):
            e, g = lax.div(q, 12), lax.div(q, 14)
            i = q + 2 * lax.div(q, 6) * (1 - e) - 6 * (e - g)
            yy = lax.div(i, n_tp)
            m = lax.div(lax.rem(i, n_tp), 2)
            off = lax.div(m * (m + 1), 2)
            return yy, lax.rem(x + off, n_x) * 2 + lax.rem(i, 2)

        def up(n, blk, m0, m1, event=None):
            def loads(idx):
                yy, tt = block(blk(idx))
                s = lax.rem(idx, NB)
                return [
                    pltpu.make_async_copy(
                        u_ref.at[yy, tt, pl.ds(p * lr, lr), :], ub.at[s, pl.ds(p * lr, lr), :], ld_sem.at[s, p]
                    )
                    for p in range(R // lr)
                ]

            for i in range(min(NB - 1, n)):
                for cp in loads(i):
                    cp.start()

            @pl.loop(0, n)
            def _(idx):
                if event is not None:
                    event(idx)

                @pl.when(idx + NB - 1 < n)
                def _():
                    for cp in loads(idx + NB - 1):
                        cp.start()

                for cp in loads(idx):
                    cp.wait()
                yy, tt = block(blk(idx))
                rows = pl.ds(pl.multiple_of((yy * n_tp + tt) * R, 16), R)

                @pl.loop(m0(idx), m1(idx))
                def _(m):
                    k = kseq(m)
                    pre = jnp.dot(ub[lax.rem(idx, NB)], wb[k], preferred_element_type=F32)
                    h[rows, cols(k, cf)] = jax.nn.gelu(pre, approximate=True).astype(BF16)

        def s_event(m):
            s_copy(sseq(m)).wait_recv()
            f_copy(sseq(m)).start()

        def w_ready(m):
            k = kseq(m)
            d_copy(k).wait_recv()
            f_recv(k).wait_recv()

        def same(v):
            return lambda idx: v

        def straight(idx):
            return idx

        s_event(0)
        s_event(1)
        for m in range(2, K1):
            d_copy(((m + 1) % 2) * 3 + m // 2).start()
        u_near(0, 0)
        u_pair(0).wait_recv()
        u_start(1, 0)
        u_sib(1, 0).start()
        u_near(0, 1)
        u_pair(1).wait_recv()
        u_start(1, 1)
        for d in range(2):
            u_fwd(0, d).start()
        u_sib(1, 1).start()
        u_near(1, 0)
        for i in range(6):
            u_sib(0, i).wait_recv()
        for i in range(2):
            u_sib(1, i).wait_recv()
        for k in range(K1):
            own_w(k).wait()
        for i in range(2):
            u_store(i).wait()
            u_pair(i).wait_send()
            u_sib(0, i).wait_send()
            for d in range(2):
                u_copy(0, d, i).wait_send()

        w_ready(0)
        w_ready(1)

        def event1(idx):
            @pl.when(idx == 5)
            def _():
                s_event(2)

        up(8, straight, same(0), same(2), event1)
        s_event(3)
        u_near(1, 1)
        for d in range(2):
            u_fwd(1, d).start()
        for i in range(2, 6):
            u_sib(1, i).wait_recv()
        up(4, lambda idx: idx + 8, same(0), same(2))
        s_event(4)
        w_ready(2)
        up(12, straight, same(2), same(3))
        s_event(5)
        for j in range(SLOTS):
            wo_copy(j).start()
        w_ready(3)

        def event2(idx):
            @pl.when(idx == 5)
            def _():
                u_far(0)

        up(12, straight, same(3), same(4), event2)
        w_ready(4)
        for i in range(6, 8):
            u_sib(0, i).wait_recv()

        def first2(idx):
            return lax.div(25 - idx, 24)

        def last_block(idx):
            g = lax.div(idx, 20)
            return idx - 2 + 14 * first2(idx) - 12 * (lax.div(idx, 14) - g) - 6 * g

        def last_event(idx):
            @pl.when(idx == 8)
            def _():
                w_ready(5)

            @pl.when(idx == 12)
            def _():
                u_far(1)

            @pl.when(idx == 15)
            def _():
                fetch(0)

            @pl.when(idx == 18)
            def _():
                for i in range(6, 8):
                    u_sib(1, i).wait_recv()

        up(
            24,
            last_block,
            lambda idx: (1 - first2(idx)) * (4 + lax.div(idx, 14)) - 5 * lax.div(idx, 22),
            lambda idx: 5 + lax.div(idx + 16, 24),
            last_event,
        )

        for yy in range(2):
            for d in range(2):
                u_fwd(yy, d).wait_send()
                if yy == 1:
                    for part in range(2):
                        u_copy(yy, d, part).wait_send()
            for i in range(2 * (1 - yy), 8):
                u_sib(yy, i).wait_send()

    pl.run_scoped(phase1, pltpu.VMEM((NB, R, D), BF16))

    for k in range(K1):
        f_copy(k).wait_send()
        d_copy(k).wait_send()
        s_copy(k).wait_send()

    def phase2(own, sibst):
        def sib_copy(j, yy):
            w = narrow(j)
            src = sibst.at[yy, :, :, w]
            return remote(src, sibr.at[s2(j), yy, :, :, w], sb_s.at[yy], sb_r.at[s2(j), yy], sib)

        def yey_copy(j):
            w = narrow(j)
            src = own.at[s4(j), 1, :, pl.ds(RX, R - RX), w]
            return remote(src, yey.at[s4(j), :, :, w], yey_s.at[s2(j)], yey_r.at[s4(j)], pair)

        def yex_copy(j):
            w = narrow(j)
            return remote(own.at[s4(j), 1, x, pl.ds(0, RX), w], yex.at[s4(j), :, w], yex_s.at[s2(j)], yex_r.at[s4(j)], pair)

        def fx_copy(j, d):
            w = narrow(j)
            src = own.at[s4(j), :, xf, pl.ds(d * hx, hx), w]
            return remote(src, fx.at[s4(j), d, :, :, w], fx_s.at[s2(j), d], fx_r.at[s4(j), d], xnb[d])

        def nx_copy(j, d):
            w = narrow(j)
            src = own.at[s4(j), :, (xr, xl)[d], pl.ds(0, RX), w]
            return remote(src, nx.at[s4(j), d, :, :, w], nx_s.at[s2(j), d], nx_r.at[s4(j), d], xnb[d])

        def fy_copy(j, d):
            w = narrow(j)
            src = own.at[s4(j), 0, xf, pl.ds(RX + d * hy, hy), w]
            return remote(src, fy.at[s4(j), d, :, w], fy_s.at[s2(j), d], fy_r.at[s4(j), d], xnb[d])

        def ny_copy(j, d):
            w = narrow(j)
            src = own.at[s4(j), 0, (xr, xl)[d], pl.ds(RX, R - RX), w]
            return remote(src, ny.at[s4(j), d, :, w], ny_s.at[s2(j), d], ny_r.at[s4(j), d], xnb[d])

        def out_copy(j):
            return pltpu.make_async_copy(hid_v.at[:, dcols(j)], out_ref.at[:, dcols(j)], out_sem.at[j])

        def when_static(cond, fn):
            if isinstance(cond, bool):
                if cond:
                    fn()
            else:
                pl.when(cond)(fn)

        def send(copy, j, *a):
            when_static(j >= 2, lambda: copy(j - 2, *a).wait_send())
            copy(j, *a).start()

        def down(j):
            W = slice(0, width(j))
            for cp in w2_loads(j):
                cp.wait()

            if isinstance(j, int):
                if j < N:
                    fetch(j + 1)
            else:
                pl.when(j + 1 < N - 1)(lambda: fetch(j + 1))
                pl.when(j + 1 == N - 1)(lambda: fetch(N - 1))

            def part(yy, xx, cc):
                rows = pl.ds(pl.multiple_of((yy * n_tp + xx * 2 + cc) * R, 16), R)
                return jnp.dot(h[rows, :], w2b[s2(j), :, W], preferred_element_type=F32)

            for yy in (1, 0):
                when_static(j >= 1, lambda: sib_copy(j - 1, yy).wait_send())

                @pl.loop(0, n_x)
                def _(xx):
                    sibst[yy, xx, :, W] = part(yy, xx, 1 - c)

                sib_copy(j, yy).start()

            @pl.loop(0, 2 * n_x)
            def _(i):
                yy, xx = 1 - lax.div(i, n_x), lax.rem(i, n_x)
                own[s4(j), yy, xx, :, W] = part(yy, xx, c)

        def stage1(j):
            W = slice(0, width(j))
            for yy in (1, 0):
                sib_copy(j, yy).wait_recv()

                @pl.loop(0, n_x)
                def _(xx):
                    own[s4(j), yy, xx, :, W] = own[s4(j), yy, xx, :, W] + sibr[s2(j), yy, xx, :, W]

                if yy == 1:
                    send(yey_copy, j)
            for d in range(2):
                send(fx_copy, j, d)

        def stage2(j):
            s, W = s4(j), slice(0, width(j))
            for d in range(2):
                fx_copy(j, d).wait_recv()
                b, rows = (xr, xl)[d], slice(d * hx, (d + 1) * hx)
                for yy in range(2):
                    own[s, yy, b, rows, W] = own[s, yy, b, rows, W] + fx[s, d, yy, :, W]
            for d in range(2):
                send(nx_copy, j, d)
            yey_copy(j).wait_recv()

            @pl.loop(0, n_x)
            def _(i):
                own[s, 0, i, RX:, W] = own[s, 0, i, RX:, W] + yey[s, i, :, W]

            for d in range(2):
                send(fy_copy, j, d)

        def stage3(j):
            s, W = s4(j), slice(0, width(j))
            for d in range(2):
                fy_copy(j, d).wait_recv()
                b, rows = (xr, xl)[d], slice(RX + d * hy, RX + (d + 1) * hy)
                own[s, 0, b, rows, W] = own[s, 0, b, rows, W] + fy[s, d, :, W]
            for d in range(2):
                ny_copy(j, d).start()
            for d in range(2):
                nx_copy(j, d).wait_recv()
            for yy in (1, 0):
                own[s, yy, x, :RX, W] = own[s, yy, x, :RX, W] + nx[s, 0, yy, :, W] + nx[s, 1, yy, :, W]
            yex_copy(j).start()

        def stage4(j):
            s, W = s4(j), slice(0, width(j))
            for d in range(2):
                ny_copy(j, d).wait_recv()
            lo = own[s, 0, x, RX:, W] + ny[s, 0, :, W] + ny[s, 1, :, W]
            hid_v[RX:, dcols(j)] = (hid_v[RX:, dcols(j)].astype(F32) + lo).astype(BF16)
            yex_copy(j).wait_recv()
            hi = own[s, 0, x, :RX, W] + yex[s, :, W]
            hid_v[:RX, dcols(j)] = (hid_v[:RX, dcols(j)].astype(F32) + hi).astype(BF16)
            out_copy(j).start()
            yex_copy(j).wait_send()
            for d in range(2):
                ny_copy(j, d).wait_send()

        @pl.loop(0, N - 1)
        def _(j):
            @pl.when(j + SLOTS < N)
            def _():
                wo_copy(j + SLOTS).start()

            down(j)
            stage1(j)
            pl.when(j >= 1)(lambda: stage2(j - 1))
            pl.when(j >= 2)(lambda: stage3(j - 2))
            pl.when(j >= 3)(lambda: stage4(j - 3))

        for j in range(N - 1, N + 4):
            if j <= N:
                down(j)
                stage1(j)
            for lag, stage in ((1, stage2), (2, stage3), (3, stage4)):
                if j - lag <= N:
                    stage(j - lag)

        for yy in range(2):
            sib_copy(N, yy).wait_send()
        for j in (N - 1, N):
            yey_copy(j).wait_send()
            for d in range(2):
                for copy in (fx_copy, nx_copy, fy_copy):
                    copy(j, d).wait_send()

        @pl.loop(0, N)
        def _(j):
            wo_copy(j).wait_send()

        @pl.loop(0, N - 1)
        def _(j):
            out_copy(j).wait()

        for j in (N - 1, N):
            out_copy(j).wait()

    pl.run_scoped(phase2, pltpu.VMEM((SLOTS, 2, n_x, R, cd), F32), pltpu.VMEM((2, n_x, R, cd), F32))


def make_local(n_tp, n_y, N):
    def local_mlp(hidden, ln_scale, w_in, w_out):
        R, D = hidden.shape
        sub = w_out.shape[0]
        cd = D // N
        n_x = n_tp // 2
        RX = split_rows(R)
        any_spec = pl.BlockSpec(memory_space=pl.ANY)
        dma = pltpu.SemaphoreType.DMA
        vm = pltpu.VMEM
        S = SLOTS
        out, _, _ = pl.pallas_call(
            functools.partial(mlp_kernel, n_tp, n_y, N),
            out_shape=(
                jax.ShapeDtypeStruct((R, D), BF16),
                jax.ShapeDtypeStruct((2, n_tp, R, D), BF16),
                jax.ShapeDtypeStruct((sub, D), BF16),
            ),
            in_specs=[any_spec, pl.BlockSpec(memory_space=vm), any_spec, any_spec],
            out_specs=(any_spec, any_spec, any_spec),
            scratch_shapes=[
                vm((6, D, sub // 3), BF16),
                vm((2 * n_tp * R, 2 * sub), BF16),
                vm((2, 2 * sub, cd), BF16),
                vm((R, D), BF16),
                vm((2, 2, n_x, R, cd), F32),
                vm((S, n_x, R - RX, cd), F32),
                vm((S, 2, 2, RX // 2, cd), F32),
                vm((S, 2, 2, RX, cd), F32),
                vm((S, 2, (R - RX) // 2, cd), F32),
                vm((S, 2, R - RX, cd), F32),
                vm((S, RX, cd), F32),
                dma((2,)), dma((2,)), dma((NB, 4)), dma((6,)), dma((2, 2)), dma((N + 1,)),
                dma((6,)), dma((6,)), dma((6,)), dma((6,)), dma((6,)), dma((6,)), dma((N,)), dma((N,)),
                dma((2,)), dma((2,)), dma((2, 2, 2)), dma((2, 2, 2)), dma((2, 2)), dma((2, 2)), dma((2, 8)), dma((2, 8)),
                dma((2,)), dma((2, 2)), dma((2,)), dma((S,)), dma((2, 2)), dma((S, 2)), dma((2, 2)), dma((S, 2)),
                dma((2, 2)), dma((S, 2)), dma((2, 2)), dma((S, 2)), dma((2,)), dma((S,)),
            ],
            compiler_params=pltpu.CompilerParams(
                collective_id=0, has_side_effects=True, vmem_limit_bytes=67043328
            ),
            cost_estimate=pl.CostEstimate(
                flops=4 * n_tp * R * D * w_in.shape[1], bytes_accessed=8 * D * w_in.shape[1], transcendentals=0
            ),
            name="mlp",
        )(hidden, ln_scale.reshape(1, D), w_in, w_out)
        return out

    return local_mlp


def solution(mesh):
    return jax.shard_map(
        make_local(mesh.shape["tp"], mesh.shape["fsdp"], CHUNKS),
        mesh=mesh,
        in_specs=(P(("data", "fsdp", "tp"), None), P(None), P("fsdp", "tp"), P(("tp", "fsdp"), None)),
        out_specs=P(("data", "fsdp", "tp"), None),
        check_vma=False,
    )
```
